32 devices in a mesh: section: 4 (over x, core), tensor: 4 (over z), dp: 2 (over y).
Axes of the slice: x: 2, y: 2, z: 4, core: 2. Of those that a mesh axis runs over, the one named last changes fastest.
Arguments:
- layer_in: bfloat16 [2, 2, 4, 2, 128, 2560], P(None, None, 'section', 'dp', 'tensor'), may hold values from -6 to 6
- carry_in: bfloat16 [2, 4, 2, 128, 2560], P(None, 'section', 'dp', 'tensor'), may hold values from -6 to 6
- top_grad: bfloat16 [1, 2, 128, 2560], P(None, 'dp', 'tensor'), may hold values from -6 to 6
- w_qkv: bfloat16 [2, 4, 2560, 2560], P(None, 'section', None, 'tensor'), may hold values from -1 to 1
- w_out: bfloat16 [2, 4, 2048, 2560], P(None, 'section', 'tensor'), may hold values from -0.125 to 0.125
- gain: float32 [2, 4, 2560], P(None, 'section'), may hold values from 0.5 to 1.5
Outputs:
- unit_grads: bfloat16 [2, 2, 4, 2, 128, 2560], P(None, None, 'section', 'dp', 'tensor')
- grad_qkv: bfloat16 [2, 4, 2560, 2560], P(None, 'section', 'dp', 'tensor')
- grad_out: bfloat16 [2, 4, 2048, 2560], P(None, 'section', ('tensor', 'dp'))
- grad_gain: float32 [2, 4, 2560], P(None, 'section')
The draws below stay inside these ranges and needn't reach their ends.
All inputs are finite; a program needn't handle non-finite values.
Results may differ from the reference program's by a relative error of at most 0.022.
The reference program's roundings to bfloat16 on the way count: a program that leaves them out, or rounds other values in their place, can miss the bound.
Values may be sent and summed in bfloat16 or wider, within the bound.
A program may use at most 128 MiB of HBM per device.

```python
import math
import jax
import jax.numpy as jnp
from jax import lax

D = 2560
KV = 4
HD = 64
SEQ = 128
TICKS = 2
GROUP = 8
HQ = 2048
QKV = 2560
SECTIONS = 4
REPLICAS = 2
N_TENSOR = 4


def draw_w_qkv(key, part):
    draw_shape = (2, SECTIONS, D, KV, GROUP + 2, HD)
    entries = jax.random.normal(key, draw_shape, jnp.float32) / jnp.sqrt(jnp.float32(D))
    return jnp.clip(entries, -1.0, 1.0).reshape(2, SECTIONS, D, KV * (GROUP + 2) * HD).astype(jnp.bfloat16)


def level_of(stream_key, shape, pieces, smallest, largest):
    def one(axis_at, parts):
        steps = jax.random.uniform(jax.random.fold_in(jax.random.fold_in(stream_key, 6), axis_at), (parts,), jnp.float32, smallest / len(pieces), largest / len(pieces))
        return jnp.repeat(jnp.exp(steps), shape[axis_at] // parts).reshape((-1,) + (1,) * (len(shape) - axis_at - 1))

    factor_of = one(*pieces[0])
    for cut in pieces[1:]:
        factor_of = factor_of * one(*cut)
    return factor_of


def gaussian(own_key, extent, spread, most, cuts=(), kind=jnp.bfloat16):
    values = spread * jax.random.normal(own_key, extent, jnp.float32)
    if cuts:
        values = values * level_of(own_key, extent, cuts, -0.22, 0.18)
    return jnp.clip(values, -most, most).astype(kind)


def setup_inputs(seed: int = 0) -> dict:
    arg_keys = jax.random.split(jax.random.key(seed), 7)
    return {
        "layer_in": gaussian(arg_keys[0], (TICKS, 2, SECTIONS, REPLICAS, SEQ, D), 1.0, 6.0, ((2, 4), (3, 2), (4, 4))),
        "carry_in": gaussian(arg_keys[1], (2, SECTIONS, REPLICAS, SEQ, D), 1.0, 6.0, ((1, 4), (2, 2), (3, 4))),
        "top_grad": gaussian(arg_keys[2], (TICKS - 1, REPLICAS, SEQ, D), 1.0, 6.0, ((1, 2), (2, 4))),
        "w_qkv": draw_w_qkv(jax.random.fold_in(arg_keys[6], 71), 0),
        "w_out": gaussian(arg_keys[4], (2, SECTIONS, HQ, D), HQ ** -0.5, 0.125, ((1, 4), (2, 4))),
        "gain": jnp.clip(1.0 + 0.1 * jax.random.normal(arg_keys[5], (2, SECTIONS, D), jnp.float32), 0.5, 1.5),
    }


epsilon = 1e-06
rope_base = 1000000.0

def rope_tables(length, head_width):
    half_width = head_width // 2
    exponent = jnp.arange(half_width, dtype=jnp.float32) * (2.0 / head_width)
    frequency = rope_base ** (-exponent)
    angle = jnp.arange(length, dtype=jnp.float32)[:, None] * frequency[None, :]
    return (jnp.cos(angle), jnp.sin(angle))

def rotate(values, cosine_table, sine_table, direction):
    half_width = values.shape[-1] // 2
    table_shape = (values.shape[0],) + (1,) * (values.ndim - 2) + (half_width,)
    cosine = cosine_table.reshape(table_shape)
    sine_part = direction * sine_table.reshape(table_shape)
    lower_half = values[..., :half_width]
    upper_half = values[..., half_width:]
    return jnp.concatenate([lower_half * cosine - upper_half * sine_part, upper_half * cosine + lower_half * sine_part], axis=-1)

def layer_backward(layer_rows, grad_output, weight_qkv, weight_out, gain_row):
    length = layer_rows.shape[0]
    cosine_table, sine_table = rope_tables(length, HD)
    inputs_float = layer_rows.astype(jnp.float32)
    inverse = lax.rsqrt(lax.optimization_barrier(jnp.mean(inputs_float * inputs_float, axis=-1, keepdims=True)) + epsilon)
    unit_rows = inputs_float * inverse
    normed = (unit_rows * gain_row).astype(jnp.bfloat16)
    projected = jnp.dot(normed, weight_qkv, preferred_element_type=jnp.float32).reshape(length, KV, GROUP + 2, HD)
    query_rot = rotate(projected[:, :, :GROUP], cosine_table, sine_table, 1.0).astype(jnp.bfloat16)
    key_rot = rotate(projected[:, :, GROUP], cosine_table, sine_table, 1.0).astype(jnp.bfloat16)
    value_rows = projected[:, :, GROUP + 1].astype(jnp.bfloat16)
    query_float = query_rot.astype(jnp.float32)
    key_float = key_rot.astype(jnp.float32)
    value_float = value_rows.astype(jnp.float32)
    score_scale = 1.0 / math.sqrt(HD)
    scores = jnp.einsum('tkgd,ukd->kgtu', query_float, key_float) * score_scale
    causal_mask = jnp.arange(length)[:, None] >= jnp.arange(length)[None, :]
    scores = jnp.where(causal_mask, scores, -1e+30)
    exponentials = jnp.exp(scores - lax.optimization_barrier(jnp.max(scores, axis=-1, keepdims=True)))
    softmax_rows = exponentials / lax.optimization_barrier(jnp.sum(exponentials, axis=-1, keepdims=True))
    softmax_low = softmax_rows.astype(jnp.bfloat16)
    softmax_float = softmax_low.astype(jnp.float32)
    attended = jnp.einsum('kgtu,ukd->tkgd', softmax_float, value_float).astype(jnp.bfloat16).reshape(length, HQ)
    grad_attended = jnp.dot(grad_output, weight_out.T, preferred_element_type=jnp.float32).astype(jnp.bfloat16)
    grad_heads = grad_attended.reshape(length, KV, GROUP, HD).astype(jnp.float32)
    grad_softmax = jnp.einsum('tkgd,ukd->kgtu', grad_heads, value_float)
    row_total = lax.optimization_barrier(jnp.sum(softmax_rows * grad_softmax, axis=-1, keepdims=True))
    grad_scores = (softmax_rows * (grad_softmax - row_total) * score_scale).astype(jnp.bfloat16)
    grad_score_float = grad_scores.astype(jnp.float32)
    grad_value = jnp.einsum('kgtu,tkgd->ukd', softmax_float, grad_heads)
    grad_query = rotate(jnp.einsum('kgtu,ukd->tkgd', grad_score_float, key_float), cosine_table, sine_table, -1.0)
    grad_key = rotate(jnp.einsum('kgtu,tkgd->ukd', grad_score_float, query_float), cosine_table, sine_table, -1.0)
    grad_projected = jnp.concatenate([grad_query, grad_key[:, :, None], grad_value[:, :, None]], axis=2)
    grad_projected = grad_projected.reshape(length, QKV).astype(jnp.bfloat16)
    block_width = QKV // N_TENSOR
    grad_normed = jnp.zeros((length, D), jnp.float32)
    for column_block in range(N_TENSOR):
        lower = column_block * block_width
        block_term = jnp.dot(grad_projected[:, lower:lower + block_width], weight_qkv[:, lower:lower + block_width].T, preferred_element_type=jnp.float32)
        grad_normed = grad_normed + block_term.astype(jnp.bfloat16).astype(jnp.float32)
    grad_unit = grad_normed * gain_row
    grad_rows = inverse * (grad_unit - unit_rows * lax.optimization_barrier(jnp.mean(grad_unit * unit_rows, axis=-1, keepdims=True)))
    grad_input = (grad_output.astype(jnp.float32) + grad_rows).astype(jnp.bfloat16)
    grad_scale = lax.optimization_barrier(jnp.sum(grad_normed * unit_rows, axis=0))
    grad_wqkv = jnp.dot(normed.T, grad_projected, preferred_element_type=jnp.float32)
    grad_wout = jnp.dot(attended.T, grad_output, preferred_element_type=jnp.float32)
    return (grad_input, grad_wqkv, grad_wout, grad_scale)

def reference(layer_in, carry_in, top_grad, w_qkv, w_out, gain):
    ticks = layer_in.shape[0]
    sections = layer_in.shape[2]
    per_replica = (jnp.moveaxis(layer_in, 3, 0), jnp.moveaxis(carry_in, 2, 0), jnp.moveaxis(top_grad, 1, 0))

    def one_replica(totals, slices):
        layer_rows, carried, fresh_grads = slices
        sum_qkv = jnp.zeros(w_qkv.shape, jnp.float32)
        sum_out = jnp.zeros(w_out.shape, jnp.float32)
        gain_total = totals[2]
        produced = {}
        per_tick = []
        for position in range(ticks):
            current = {}
            for member in (1, 0):
                for section_index in range(sections):
                    if position == 0:
                        incoming = carried[member, section_index]
                    elif member == 1 and section_index == 0:
                        incoming = fresh_grads[position - 1]
                    elif member == 1:
                        incoming = produced[1, section_index - 1]
                    elif section_index == sections - 1:
                        incoming = produced[1, section_index]
                    else:
                        incoming = produced[0, section_index + 1]
                    outcome = layer_backward(layer_rows[position, member, section_index], incoming, w_qkv[member, section_index], w_out[member, section_index], gain[member, section_index])
                    current[member, section_index] = outcome[0]
                    sum_qkv = sum_qkv.at[member, section_index].add(outcome[1])
                    sum_out = sum_out.at[member, section_index].add(outcome[2])
                    gain_total = gain_total.at[member, section_index].add(outcome[3])
            produced = current
            per_tick.append(jnp.stack([jnp.stack([current[member, index] for index in range(sections)]) for member in (0, 1)]))
        new_qkv = totals[0] + sum_qkv.astype(jnp.bfloat16).astype(jnp.float32)
        new_out = totals[1] + sum_out.astype(jnp.bfloat16).astype(jnp.float32)
        return ((new_qkv, new_out, gain_total), jnp.stack(per_tick))
    start_totals = (jnp.zeros(w_qkv.shape, jnp.float32), jnp.zeros(w_out.shape, jnp.float32), jnp.zeros(gain.shape, jnp.float32))
    totals, grads_all = lax.scan(one_replica, start_totals, per_replica)
    unit_grads = jnp.moveaxis(grads_all, 0, 3)
    return (unit_grads, totals[0].astype(jnp.bfloat16), totals[1].astype(jnp.bfloat16), totals[2])
```

```python
import math

import jax
import jax.numpy as jnp
from jax import lax
from jax.sharding import PartitionSpec as P

HD = 64
GROUP = 8

epsilon = 1e-06
rope_base = 1000000.0


contract_rows = (((0,), (0,)), ((), ()))
contract_cols = (((1,), (1,)), ((), ()))


def from_behind(value, axis, steps):
    count = lax.axis_size(axis)
    first, last = (max(0, -steps), min(count, count - steps))
    return lax.ppermute(value, axis, [(source, source + steps) for source in range(first, last)])


def from_ahead(value, axis, steps):
    count = lax.axis_size(axis)
    return lax.ppermute(value, axis, [((i + steps) % count, i) for i in range(count)])


def rope_tables(positions, head_width):
    half_width = head_width // 2
    exponent = jnp.arange(half_width, dtype=jnp.float32) * (2.0 / head_width)
    frequency = rope_base ** (-exponent)
    angle = positions.astype(jnp.float32)[:, None] * frequency[None, :]
    return (jnp.cos(angle), jnp.sin(angle))


def rotate(values, cosine_table, sine_table, direction):
    half_width = values.shape[-1] // 2
    table_shape = (values.shape[0],) + (1,) * (values.ndim - 2) + (half_width,)
    cosine = cosine_table.reshape(table_shape)
    sine_part = direction * sine_table.reshape(table_shape)
    lower_half = values[..., :half_width]
    upper_half = values[..., half_width:]
    return jnp.concatenate(
        [
            lower_half * cosine - upper_half * sine_part,
            upper_half * cosine + lower_half * sine_part,
        ],
        axis=-1,
    )


def unit_compute(normed, grad_full, w_qkv, w_out, tables, mask):
    length = normed.shape[0]
    kv_local = w_out.shape[0] // (GROUP * HD)
    cosine_table, sine_table = tables
    score_scale = 1.0 / math.sqrt(HD)
    projected = jnp.dot(normed, w_qkv, preferred_element_type=jnp.float32)
    projected = projected.reshape(length, kv_local, GROUP + 2, HD)
    query_rot = rotate(projected[:, :, :GROUP], cosine_table, sine_table, 1.0).astype(jnp.bfloat16)
    key_rot = rotate(projected[:, :, GROUP], cosine_table, sine_table, 1.0).astype(jnp.bfloat16)
    value_rows = projected[:, :, GROUP + 1].astype(jnp.bfloat16)
    f32 = dict(preferred_element_type=jnp.float32)
    scores = jnp.einsum("tkgd,ukd->kgtu", query_rot, key_rot, **f32) * score_scale
    scores = jnp.where(mask, scores, -1e30)
    exponentials = jnp.exp(scores - jnp.max(scores, axis=-1, keepdims=True))
    softmax_rows = exponentials / jnp.sum(exponentials, axis=-1, keepdims=True)
    softmax_low = softmax_rows.astype(jnp.bfloat16)
    attended = jnp.einsum("kgtu,ukd->tkgd", softmax_low, value_rows, **f32)
    attended = attended.astype(jnp.bfloat16).reshape(length, kv_local * GROUP * HD)
    grad_attended = lax.dot_general(grad_full, w_out, contract_cols, **f32).astype(jnp.bfloat16)
    grad_heads = grad_attended.reshape(length, kv_local, GROUP, HD)
    grad_softmax = jnp.einsum("tkgd,ukd->kgtu", grad_heads, value_rows, **f32)
    row_total = jnp.sum(softmax_rows * grad_softmax, axis=-1, keepdims=True)
    grad_scores = (softmax_rows * (grad_softmax - row_total) * score_scale).astype(jnp.bfloat16)
    grad_value = jnp.einsum("kgtu,tkgd->ukd", softmax_low, grad_heads, **f32)
    grad_query = rotate(
        jnp.einsum("kgtu,ukd->tkgd", grad_scores, key_rot, **f32), cosine_table, sine_table, -1.0
    )
    grad_key = rotate(
        jnp.einsum("kgtu,tkgd->ukd", grad_scores, query_rot, **f32), cosine_table, sine_table, -1.0
    )
    grad_projected = jnp.concatenate(
        [grad_query, grad_key[:, :, None], grad_value[:, :, None]], axis=2
    )
    grad_projected = grad_projected.reshape(length, kv_local * (GROUP + 2) * HD)
    grad_projected = grad_projected.astype(jnp.bfloat16)
    partial = lax.dot_general(grad_projected, w_qkv, contract_cols, **f32).astype(jnp.bfloat16)
    return attended, grad_projected, partial


def local(layer_in, carry_in, top_grad, w_qkv, w_out, gain):
    ticks = layer_in.shape[0]
    own = layer_in.shape[4]
    n_tensor = lax.axis_size("tensor")
    n_dp = lax.axis_size("dp")
    me_tensor = lax.axis_index("tensor")
    me_dp = lax.axis_index("dp")
    section_index = lax.axis_index("section")
    at_first = section_index == 0
    at_last = section_index == lax.axis_size("section") - 1
    owners = (me_tensor + jnp.arange(n_tensor)) % n_tensor
    positions = (owners[:, None] * own + jnp.arange(own)[None, :]).reshape(-1)
    tables = rope_tables(positions, HD)
    mask = positions[:, None] >= positions[None, :]
    layer_rows = layer_in[:, :, 0, 0]
    carried = carry_in[:, 0, 0]
    fresh_grads = top_grad[:, 0]
    weight_qkv = w_qkv[:, 0]
    weight_out = w_out[:, 0]
    gain_rows = gain[:, 0]

    def gather(value):
        return jnp.concatenate(
            [value] + [from_ahead(value, "tensor", k) for k in range(1, n_tensor)], axis=0
        )

    def scatter_sum(partial):
        total = partial[:own].astype(jnp.float32)
        for k in range(1, n_tensor):
            chunk = partial[k * own : (k + 1) * own]
            total = total + from_ahead(chunk, "tensor", -k).astype(jnp.float32)
        return total

    def columns_of(value, index):
        width = value.shape[1] // n_dp
        return lax.dynamic_slice_in_dim(value, index * width, width, axis=1)

    def exchange(value, cut):
        if cut:
            return [columns_of(value, me_dp)] + [
                from_ahead(columns_of(value, (me_dp - k) % n_dp), "dp", k) for k in range(1, n_dp)
            ]
        return [value] + [from_ahead(value, "dp", k) for k in range(1, n_dp)]

    members = (1, 0)
    unit_rows, inverse, normed = {}, {}, {}
    for t in range(ticks):
        for m in members:
            rows = layer_rows[t, m].astype(jnp.float32)
            inverse[t, m] = lax.rsqrt(jnp.mean(rows * rows, axis=-1, keepdims=True) + epsilon)
            unit_rows[t, m] = rows * inverse[t, m]
            normed[t, m] = (unit_rows[t, m] * gain_rows[m]).astype(jnp.bfloat16)
    inputs = [carried[0], carried[1]]
    factors = {}
    per_tick = []
    gain_totals = [0.0, 0.0]
    for t in range(ticks):
        outcome = [None, None]
        for m in members:
            dy = inputs[m]
            full_normed = gather(normed[t, m])
            full_grad = gather(dy)
            attended, grad_projected, partial = unit_compute(
                full_normed, full_grad, weight_qkv[m], weight_out[m], tables, mask
            )
            factors[t, m] = (
                exchange(full_normed, True),
                exchange(grad_projected, False),
                exchange(attended, True),
                exchange(full_grad, False),
            )
            grad_normed = scatter_sum(partial)
            grad_unit = grad_normed * gain_rows[m]
            unit = unit_rows[t, m]
            grad_rows = inverse[t, m] * (
                grad_unit - unit * jnp.mean(grad_unit * unit, axis=-1, keepdims=True)
            )
            outcome[m] = (dy.astype(jnp.float32) + grad_rows).astype(jnp.bfloat16)
            gain_totals[m] = gain_totals[m] + jnp.sum(grad_normed * unit, axis=0)
        if t + 1 < ticks:
            upward = from_behind(outcome[1], "section", 1)
            downward = from_behind(outcome[0], "section", -1)
            inputs = [
                jnp.where(at_last, outcome[1], downward),
                jnp.where(at_first, fresh_grads[t], upward),
            ]
        per_tick.append(jnp.stack(outcome))

    def weight_grad(m, left, right):
        total = None
        for k in range(n_dp):
            a = jnp.concatenate([factors[t, m][left][k] for t in range(ticks)], axis=0)
            b = jnp.concatenate([factors[t, m][right][k] for t in range(ticks)], axis=0)
            part = lax.dot_general(a, b, contract_rows, preferred_element_type=jnp.float32)
            part = part.astype(jnp.bfloat16).astype(jnp.float32)
            total = part if total is None else total + part
        return total.astype(jnp.bfloat16)

    grad_qkv = jnp.stack([weight_grad(m, 0, 1) for m in (0, 1)])
    grad_out = jnp.stack([weight_grad(m, 2, 3) for m in (0, 1)])
    gain_total = lax.psum(jnp.stack(gain_totals), ("tensor", "dp"))
    return (
        jnp.stack(per_tick)[:, :, None, None],
        grad_qkv[:, None],
        grad_out[:, None],
        gain_total[:, None],
    )


def solution(mesh):
    in_specs = (
        P(None, None, "section", "dp", "tensor", None),
        P(None, "section", "dp", "tensor", None),
        P(None, "dp", "tensor", None),
        P(None, "section", None, "tensor"),
        P(None, "section", "tensor", None),
        P(None, "section", None),
    )
    out_specs = (
        P(None, None, "section", "dp", "tensor", None),
        P(None, "section", "dp", "tensor"),
        P(None, "section", ("tensor", "dp"), None),
        P(None, "section", None),
    )
    return jax.shard_map(local, mesh=mesh, in_specs=in_specs, out_specs=out_specs, check_vma=False)
```

```python
import functools
import math

import jax
import jax.numpy as jnp
from jax import lax
from jax.experimental import pallas as pl
from jax.experimental.pallas import tpu as pltpu
from jax.sharding import PartitionSpec as P

HD = 64
GROUP = 8

epsilon = 1e-06
rope_base = 1000000.0


MESH = pl.DeviceIdType.MESH

contract_rows = (((0,), (0,)), ((), ()))
contract_cols = (((1,), (1,)), ((), ()))


def from_behind(value, axis, steps):
    count = lax.axis_size(axis)
    first, last = (max(0, -steps), min(count, count - steps))
    return lax.ppermute(value, axis, [(source, source + steps) for source in range(first, last)])


def from_ahead(value, axis, steps):
    count = lax.axis_size(axis)
    return lax.ppermute(value, axis, [((i + steps) % count, i) for i in range(count)])


def rope_tables(positions, head_width):
    half_width = head_width // 2
    exponent = jnp.arange(half_width, dtype=jnp.float32) * (2.0 / head_width)
    frequency = rope_base ** (-exponent)
    angle = positions.astype(jnp.float32)[:, None] * frequency[None, :]
    return (jnp.cos(angle), jnp.sin(angle))


def rotate(values, cosine_table, sine_table, direction):
    half_width = values.shape[-1] // 2
    table_shape = (values.shape[0],) + (1,) * (values.ndim - 2) + (half_width,)
    cosine = cosine_table.reshape(table_shape)
    sine_part = direction * sine_table.reshape(table_shape)
    lower_half = values[..., :half_width]
    upper_half = values[..., half_width:]
    return jnp.concatenate(
        [
            lower_half * cosine - upper_half * sine_part,
            upper_half * cosine + lower_half * sine_part,
        ],
        axis=-1,
    )


def unit_compute(normed, grad_full, w_qkv, w_out, tables, mask):
    length = normed.shape[0]
    kv_local = w_out.shape[0] // (GROUP * HD)
    cosine_table, sine_table = tables
    score_scale = 1.0 / math.sqrt(HD)
    projected = jnp.dot(normed, w_qkv, preferred_element_type=jnp.float32)
    projected = projected.reshape(length, kv_local, GROUP + 2, HD)
    query_rot = rotate(projected[:, :, :GROUP], cosine_table, sine_table, 1.0).astype(jnp.bfloat16)
    key_rot = rotate(projected[:, :, GROUP], cosine_table, sine_table, 1.0).astype(jnp.bfloat16)
    value_rows = projected[:, :, GROUP + 1].astype(jnp.bfloat16)
    f32 = dict(preferred_element_type=jnp.float32)
    scores = jnp.einsum("tkgd,ukd->kgtu", query_rot, key_rot, **f32) * score_scale
    scores = jnp.where(mask, scores, -1e30)
    exponentials = jnp.exp(scores - jnp.max(scores, axis=-1, keepdims=True))
    softmax_rows = exponentials / jnp.sum(exponentials, axis=-1, keepdims=True)
    softmax_low = softmax_rows.astype(jnp.bfloat16)
    attended = jnp.einsum("kgtu,ukd->tkgd", softmax_low, value_rows, **f32)
    attended = attended.astype(jnp.bfloat16).reshape(length, kv_local * GROUP * HD)
    grad_attended = lax.dot_general(grad_full, w_out, contract_cols, **f32).astype(jnp.bfloat16)
    grad_heads = grad_attended.reshape(length, kv_local, GROUP, HD)
    grad_softmax = jnp.einsum("tkgd,ukd->kgtu", grad_heads, value_rows, **f32)
    row_total = jnp.sum(softmax_rows * grad_softmax, axis=-1, keepdims=True)
    grad_scores = (softmax_rows * (grad_softmax - row_total) * score_scale).astype(jnp.bfloat16)
    grad_value = jnp.einsum("kgtu,tkgd->ukd", softmax_low, grad_heads, **f32)
    grad_query = rotate(
        jnp.einsum("kgtu,ukd->tkgd", grad_scores, key_rot, **f32), cosine_table, sine_table, -1.0
    )
    grad_key = rotate(
        jnp.einsum("kgtu,tkgd->ukd", grad_scores, query_rot, **f32), cosine_table, sine_table, -1.0
    )
    grad_projected = jnp.concatenate(
        [grad_query, grad_key[:, :, None], grad_value[:, :, None]], axis=2
    )
    grad_projected = grad_projected.reshape(length, kv_local * (GROUP + 2) * HD)
    grad_projected = grad_projected.astype(jnp.bfloat16)
    partial = lax.dot_general(grad_projected, w_qkv, contract_cols, **f32).astype(jnp.bfloat16)
    return attended, grad_projected, partial


def local_permutes(layer_in, carry_in, top_grad, w_qkv, w_out, gain):
    ticks = layer_in.shape[0]
    own = layer_in.shape[4]
    n_tensor = lax.axis_size("tensor")
    n_dp = lax.axis_size("dp")
    me_tensor = lax.axis_index("tensor")
    me_dp = lax.axis_index("dp")
    section_index = lax.axis_index("section")
    at_first = section_index == 0
    at_last = section_index == lax.axis_size("section") - 1
    owners = (me_tensor + jnp.arange(n_tensor)) % n_tensor
    positions = (owners[:, None] * own + jnp.arange(own)[None, :]).reshape(-1)
    tables = rope_tables(positions, HD)
    mask = positions[:, None] >= positions[None, :]
    layer_rows = layer_in[:, :, 0, 0]
    carried = carry_in[:, 0, 0]
    fresh_grads = top_grad[:, 0]
    weight_qkv = w_qkv[:, 0]
    weight_out = w_out[:, 0]
    gain_rows = gain[:, 0]

    def gather(value):
        return jnp.concatenate(
            [value] + [from_ahead(value, "tensor", k) for k in range(1, n_tensor)], axis=0
        )

    def scatter_sum(partial):
        total = partial[:own].astype(jnp.float32)
        for k in range(1, n_tensor):
            chunk = partial[k * own : (k + 1) * own]
            total = total + from_ahead(chunk, "tensor", -k).astype(jnp.float32)
        return total

    def columns_of(value, index):
        width = value.shape[1] // n_dp
        return lax.dynamic_slice_in_dim(value, index * width, width, axis=1)

    def exchange(value, cut):
        if cut:
            return [columns_of(value, me_dp)] + [
                from_ahead(columns_of(value, (me_dp - k) % n_dp), "dp", k) for k in range(1, n_dp)
            ]
        return [value] + [from_ahead(value, "dp", k) for k in range(1, n_dp)]

    members = (1, 0)
    unit_rows, inverse, normed = {}, {}, {}
    for t in range(ticks):
        for m in members:
            rows = layer_rows[t, m].astype(jnp.float32)
            inverse[t, m] = lax.rsqrt(jnp.mean(rows * rows, axis=-1, keepdims=True) + epsilon)
            unit_rows[t, m] = rows * inverse[t, m]
            normed[t, m] = (unit_rows[t, m] * gain_rows[m]).astype(jnp.bfloat16)
    inputs = [carried[0], carried[1]]
    factors = {}
    per_tick = []
    gain_totals = [0.0, 0.0]
    for t in range(ticks):
        outcome = [None, None]
        for m in members:
            dy = inputs[m]
            full_normed = gather(normed[t, m])
            full_grad = gather(dy)
            attended, grad_projected, partial = unit_compute(
                full_normed, full_grad, weight_qkv[m], weight_out[m], tables, mask
            )
            factors[t, m] = (
                exchange(full_normed, True),
                exchange(grad_projected, False),
                exchange(attended, True),
                exchange(full_grad, False),
            )
            grad_normed = scatter_sum(partial)
            grad_unit = grad_normed * gain_rows[m]
            unit = unit_rows[t, m]
            grad_rows = inverse[t, m] * (
                grad_unit - unit * jnp.mean(grad_unit * unit, axis=-1, keepdims=True)
            )
            outcome[m] = (dy.astype(jnp.float32) + grad_rows).astype(jnp.bfloat16)
            gain_totals[m] = gain_totals[m] + jnp.sum(grad_normed * unit, axis=0)
        if t + 1 < ticks:
            upward = from_behind(outcome[1], "section", 1)
            downward = from_behind(outcome[0], "section", -1)
            inputs = [
                jnp.where(at_last, outcome[1], downward),
                jnp.where(at_first, fresh_grads[t], upward),
            ]
        per_tick.append(jnp.stack(outcome))

    def weight_grad(m, left, right):
        total = None
        for k in range(n_dp):
            a = jnp.concatenate([factors[t, m][left][k] for t in range(ticks)], axis=0)
            b = jnp.concatenate([factors[t, m][right][k] for t in range(ticks)], axis=0)
            part = lax.dot_general(a, b, contract_rows, preferred_element_type=jnp.float32)
            part = part.astype(jnp.bfloat16).astype(jnp.float32)
            total = part if total is None else total + part
        return total.astype(jnp.bfloat16)

    grad_qkv = jnp.stack([weight_grad(m, 0, 1) for m in (0, 1)])
    grad_out = jnp.stack([weight_grad(m, 2, 3) for m in (0, 1)])
    gain_total = lax.psum(jnp.stack(gain_totals), ("tensor", "dp"))
    return (
        jnp.stack(per_tick)[:, :, None, None],
        grad_qkv[:, None],
        grad_out[:, None],
        gain_total[:, None],
    )


def fused(
    n, reps, ticks, sections, own,
    nrm_own, x_ref, carry, top, gain, wq_hbm, wo_hbm, cos_ref, sin_ref, bias_ref,
    out, gq_out, go_out, gain_out,
    wq, wo, nrm, dyb, gpb, attb, pnrm, pdy, pgp, patt, pb, rb, smb, qsb, kb, vb, gtot, grecv,
    w_sem, l_sem, g_send, g_recv, r_send, r_recv, s_send, s_recv, d_send, d_recv, t_send, t_recv,
):
    f32 = jnp.float32
    bf16 = jnp.bfloat16
    me = lax.axis_index("tensor")
    rep = lax.axis_index("dp")
    sec = lax.axis_index("section")
    length = n * own
    units = 2 * ticks
    hq = wo.shape[1]
    cols = wq.shape[2]
    groups = hq // (GROUP * HD)
    wn = nrm.shape[2] // reps
    wa = hq // reps
    scale = 1.0 / math.sqrt(HD)

    def tensor_at(k):
        return {"tensor": lax.rem(me + k + n, n)}

    def dp_at(k):
        return {"dp": lax.rem(rep + k + reps, reps)}

    w_copies = [
        pltpu.make_async_copy(src.at[m], dst.at[m], w_sem.at[j, m])
        for m in (1, 0)
        for j, (src, dst) in enumerate(((wq_hbm, wq), (wo_hbm, wo)))
    ]
    for c in w_copies:
        c.start()

    barrier = pltpu.get_barrier_semaphore()
    for a in range(n):
        for b in range(reps):
            if a or b:
                pl.semaphore_signal(
                    barrier, inc=1, device_id={**tensor_at(a), **dp_at(b)}, device_id_type=MESH
                )

    @pl.when(sec > 0)
    def _():
        pl.semaphore_signal(barrier, inc=1, device_id={"section": sec - 1}, device_id_type=MESH)

    @pl.when(sec < sections - 1)
    def _():
        pl.semaphore_signal(barrier, inc=1, device_id={"section": sec + 1}, device_id_type=MESH)

    neighbours = jnp.where(sec > 0, 1, 0) + jnp.where(sec < sections - 1, 1, 0)
    pl.semaphore_wait(barrier, n * reps - 1 + neighbours)

    def remote(src, dst, send, recv, where):
        return pltpu.make_async_remote_copy(
            src_ref=src, dst_ref=dst, send_sem=send, recv_sem=recv, device_id=where,
            device_id_type=MESH,
        )

    def rows(k):
        return pl.ds(k * own, own)

    def gather_copy(which, src, buf, u, k):
        return remote(
            src, buf.at[u, rows(k)], g_send.at[which, u, k], g_recv.at[which, u, k], tensor_at(-k)
        )

    def normed_copy(u, k):
        return gather_copy(0, nrm_own.at[u], nrm, u, k)

    def grad_copy(u, k):
        return gather_copy(1, dyb.at[u, rows(0)], dyb, u, k)

    def scatter_copy(u, k):
        return remote(pb.at[u, rows(k)], rb.at[u, k], r_send.at[u, k], r_recv.at[u, k], tensor_at(k))

    def dp_copy(which, u, j):
        peer = lax.rem(rep - j + reps, reps)
        nc = pl.ds(pl.multiple_of(peer * wn, 128), wn)
        ac = pl.ds(pl.multiple_of(peer * wa, 128), wa)
        src = (nrm.at[u, :, nc], dyb.at[u], gpb.at[u], attb.at[u, :, ac])[which]
        dst = (pnrm, pdy, pgp, patt)[which].at[u, j - 1]
        return remote(src, dst, d_send.at[which, u, j], d_recv.at[which, u, j], dp_at(-j))

    def section_copy(t, m):
        step = 1 if m == 1 else -1
        return remote(
            out.at[2 * t + m], dyb.at[2 * (t + 1) + m, rows(0)], s_send.at[t, m], s_recv.at[t, m],
            {"section": sec + step},
        )

    def gain_copy(a, b):
        slot = a * reps + b
        return remote(
            gtot, grecv.at[slot], t_send.at[slot], t_recv.at[slot],
            {**tensor_at(-a), **dp_at(-b)},
        )

    peers = range(1, n)
    others = range(1, reps)

    local_copies = []
    for u in range(units):
        local_copies.append(pltpu.make_async_copy(nrm_own.at[u], nrm.at[u, rows(0)], l_sem.at[u]))
    for m in (0, 1):
        local_copies.append(
            pltpu.make_async_copy(carry.at[m], dyb.at[m, rows(0)], l_sem.at[units + m])
        )
    for c in local_copies:
        c.start()
    for c in local_copies:
        c.wait()
    for m in (1, 0):
        for k in peers:
            normed_copy(m, k).start()
        for k in peers:
            grad_copy(m, k).start()
    gtot[...] = jnp.zeros_like(gtot)
    for c in w_copies:
        c.wait()

    def swap(values):
        width = values.shape[1]
        lane = lax.broadcasted_iota(jnp.int32, values.shape, 1)
        low = lax.rem(lane, HD) < HD // 2
        return jnp.where(
            low, pltpu.roll(values, width - HD // 2, 1), pltpu.roll(values, HD // 2, 1)
        )

    def dot(a, b, ca, cb):
        return lax.dot_general(a, b, (((ca,), (cb,)), ((), ())), preferred_element_type=f32)

    def stack_heads(values):
        return jnp.concatenate([values[:, h * HD : (h + 1) * HD] for h in range(GROUP)], axis=0)

    def spread_heads(values):
        return jnp.concatenate(
            [values[h * length : (h + 1) * length] for h in range(GROUP)], axis=1
        )

    span = (GROUP + 2) * HD

    def forward(u, m):
        for k in peers:
            normed_copy(u, k).wait_recv()
        for j in others:
            dp_copy(0, u, j).start()
        projected = dot(nrm[u], wq[m], 1, 0)
        rotated = (projected * cos_ref[...] + swap(projected) * sin_ref[...]).astype(bf16)
        for g in range(groups):
            at = g * span
            qs = stack_heads(rotated[:, at : at + GROUP * HD])
            key = rotated[:, at + GROUP * HD : at + (GROUP + 1) * HD]
            value = projected[:, at + (GROUP + 1) * HD : at + span].astype(bf16)
            scores = dot(qs, key, 1, 1) * scale
            scores = (scores.reshape(GROUP, length, length) + bias_ref[...][None]).reshape(
                GROUP * length, length
            )
            e = jnp.exp(scores - jnp.max(scores, axis=-1, keepdims=True))
            sm = e / jnp.sum(e, axis=-1, keepdims=True)
            smb[u, g] = sm
            qsb[u, g] = qs
            kb[u, g] = key
            vb[u, g] = value
            attended = spread_heads(dot(sm.astype(bf16), value, 1, 0).astype(bf16))
            attb[u, :, g * GROUP * HD : (g + 1) * GROUP * HD] = attended
        for j in others:
            dp_copy(3, u, j).start()

    def backward(u, m):
        for k in peers:
            grad_copy(u, k).wait_recv()
        for j in others:
            dp_copy(1, u, j).start()
        grad_att = dot(dyb[u], wo[m], 1, 1).astype(bf16)
        for g in range(groups):
            sm = smb[u, g]
            low = sm.astype(bf16)
            value = vb[u, g]
            gs = stack_heads(grad_att[:, g * GROUP * HD : (g + 1) * GROUP * HD])
            gsm = dot(gs, value, 1, 1)
            total = jnp.sum(sm * gsm, axis=-1, keepdims=True)
            gsc = (sm * (gsm - total) * scale).astype(bf16)
            g_value = dot(low, gs, 0, 0)
            g_query = spread_heads(dot(gsc, kb[u, g], 1, 0))
            g_key = dot(gsc, qsb[u, g], 0, 0)
            turned = jnp.concatenate([g_query, g_key, g_value], axis=1)
            cs = cos_ref[:, g * span : (g + 1) * span]
            sn = sin_ref[:, g * span : (g + 1) * span]
            back = turned * cs - swap(turned) * sn
            lane = lax.broadcasted_iota(jnp.int32, turned.shape, 1)
            back = jnp.where(lane < (GROUP + 1) * HD, back, turned)
            gpb[u, :, g * span : (g + 1) * span] = back.astype(bf16)
        for j in others:
            dp_copy(2, u, j).start()
        pb[u] = dot(gpb[u], wq[m], 1, 1).astype(bf16)
        for k in peers:
            scatter_copy(u, k).start()

    def finish(u, m):
        x = x_ref[u].astype(f32)
        inverse = lax.rsqrt(jnp.mean(x * x, axis=-1, keepdims=True) + epsilon)
        unit = x * inverse
        gn = pb[u, 0:own].astype(f32)
        for k in peers:
            scatter_copy(u, k).wait_recv()
            gn = gn + rb[u, k].astype(f32)
        gu = gn * gain[m]
        grad = inverse * (gu - unit * jnp.mean(gu * unit, axis=-1, keepdims=True))
        out[u] = (dyb[u, 0:own].astype(f32) + grad).astype(bf16)
        gtot[m] = gtot[m] + jnp.sum(gn * unit, axis=0, keepdims=True)

    def pair(body):
        @pl.loop(0, 2)
        def _(i):
            body(i)

    def weight_grads(m):
        def part(a_of, b_of):
            p = None
            for t in range(ticks):
                q = dot(a_of(2 * t + m), b_of(2 * t + m), 0, 0)
                p = q if p is None else p + q
            return p.astype(bf16).astype(f32)

        block = 256 if wn % 256 == 0 else 128

        @pl.loop(0, wn // block)
        def _(c):
            own_at = pl.ds(pl.multiple_of(rep * wn + c * block, 128), block)
            at = pl.ds(pl.multiple_of(c * block, 128), block)
            total = part(lambda u: nrm[u, :, own_at], lambda u: gpb[u])
            for j in others:
                total = total + part(lambda u: pnrm[u, j - 1, :, at], lambda u: pgp[u, j - 1])
            gq_out[m, at] = total.astype(bf16)

        width = dyb.shape[2]
        wide = 512 if width % 512 == 0 else 128
        att_at = pl.ds(pl.multiple_of(rep * wa, 128), wa)

        @pl.loop(0, width // wide)
        def _(c):
            at = pl.ds(pl.multiple_of(c * wide, 128), wide)
            total = part(lambda u: attb[u, :, att_at], lambda u: dyb[u, :, at])
            for j in others:
                total = total + part(lambda u: patt[u, j - 1], lambda u: pdy[u, j - 1, :, at])
            go_out[m, :, at] = total.astype(bf16)

    for t in range(ticks):

        @pl.loop(0, 2)
        def _(i):
            m = 1 - i
            u = 2 * t + m
            if t == 0:
                forward(u, m)
            backward(u, m)

        if t + 1 < ticks:
            for m in (1, 0):
                for k in peers:
                    normed_copy(2 * (t + 1) + m, k).start()
            for m in (1, 0):
                finish(2 * t + m, m)
                if m == 1:

                    @pl.when(sec < sections - 1)
                    def _():
                        section_copy(t, 1).start()

                    @pl.when(sec == sections - 1)
                    def _():
                        dyb[2 * (t + 1), 0:own] = out[2 * t + 1]

                    @pl.when(sec == 0)
                    def _():
                        dyb[2 * (t + 1) + 1, 0:own] = top[t]

                else:

                    @pl.when(sec > 0)
                    def _():
                        section_copy(t, 0).start()

            @pl.when(sec > 0)
            def _():
                section_copy(t, 1).wait_recv()

            for k in peers:
                grad_copy(2 * (t + 1) + 1, k).start()

            @pl.when(sec < sections - 1)
            def _():
                section_copy(t, 0).wait_recv()

            for k in peers:
                grad_copy(2 * (t + 1), k).start()

            @pl.loop(0, 2)
            def _(i):
                forward(2 * (t + 1) + 1 - i, 1 - i)

    last = 2 * (ticks - 1)
    for m in (1, 0):
        finish(last + m, m)
    for a in range(n):
        for b in range(reps):
            if a or b:
                gain_copy(a, b).start()
    for m in (1, 0):
        for t in range(ticks):
            for which in range(4):
                for j in others:
                    dp_copy(which, 2 * t + m, j).wait_recv()
        weight_grads(m)
    total = gtot[...]
    for a in range(n):
        for b in range(reps):
            if a or b:
                gain_copy(a, b).wait_recv()
                total = total + grecv[a * reps + b]
    gain_out[...] = total
    for u in range(units):
        for k in peers:
            normed_copy(u, k).wait_send()
            grad_copy(u, k).wait_send()
            scatter_copy(u, k).wait_send()
        for j in others:
            for which in range(4):
                dp_copy(which, u, j).wait_send()
    for t in range(ticks - 1):

        @pl.when(sec < sections - 1)
        def _():
            section_copy(t, 1).wait_send()

        @pl.when(sec > 0)
        def _():
            section_copy(t, 0).wait_send()

    for a in range(n):
        for b in range(reps):
            if a or b:
                gain_copy(a, b).wait_send()


def local(layer_in, carry_in, top_grad, w_qkv, w_out, gain):
    ticks, own, width = layer_in.shape[0], layer_in.shape[4], layer_in.shape[5]
    n = lax.axis_size("tensor")
    reps = lax.axis_size("dp")
    sections = lax.axis_size("section")
    cols, hq = w_qkv.shape[3], w_out.shape[2]
    if (width // reps) % 128 or (hq // reps) % 128 or ticks < 2:
        return local_permutes(layer_in, carry_in, top_grad, w_qkv, w_out, gain)
    length = n * own
    units = 2 * ticks
    groups = hq // (GROUP * HD)
    wn, wa = width // reps, hq // reps
    f32, bf16 = jnp.float32, jnp.bfloat16
    me = lax.axis_index("tensor")
    owners = (me + jnp.arange(n)) % n
    positions = (owners[:, None] * own + jnp.arange(own)[None, :]).reshape(-1)
    cosine, sine = rope_tables(positions, HD)
    slots = cols // HD
    cosine = jnp.tile(jnp.concatenate([cosine, cosine], axis=1), (1, slots))
    sine = jnp.tile(jnp.concatenate([-sine, sine], axis=1), (1, slots))
    bias = jnp.where(positions[:, None] >= positions[None, :], 0.0, -1e30).astype(f32)
    rows = layer_in[:, :, 0, 0]
    wide = rows.astype(f32)
    inverse = lax.rsqrt(jnp.mean(wide * wide, axis=-1, keepdims=True) + epsilon)
    normed = (wide * inverse * gain[:, 0][None, :, None, :]).astype(bf16)
    vmem = pl.BlockSpec(memory_space=pltpu.VMEM)
    hbm = pl.BlockSpec(memory_space=pl.ANY)
    dma = pltpu.SemaphoreType.DMA
    outs = pl.pallas_call(
        functools.partial(fused, n, reps, ticks, sections, own),
        out_shape=(
            jax.ShapeDtypeStruct((units, own, width), bf16),
            jax.ShapeDtypeStruct((2, wn, cols), bf16),
            jax.ShapeDtypeStruct((2, wa, width), bf16),
            jax.ShapeDtypeStruct((2, 1, width), f32),
        ),
        in_specs=[vmem] * 5 + [hbm] * 2 + [vmem] * 3,
        out_specs=(vmem,) * 4,
        scratch_shapes=[
            pltpu.VMEM((2, width, cols), bf16),
            pltpu.VMEM((2, hq, width), bf16),
            pltpu.VMEM((units, length, width), bf16),
            pltpu.VMEM((units, length, width), bf16),
            pltpu.VMEM((units, length, cols), bf16),
            pltpu.VMEM((units, length, hq), bf16),
            pltpu.VMEM((units, reps - 1, length, wn), bf16),
            pltpu.VMEM((units, reps - 1, length, width), bf16),
            pltpu.VMEM((units, reps - 1, length, cols), bf16),
            pltpu.VMEM((units, reps - 1, length, wa), bf16),
            pltpu.VMEM((units, length, width), bf16),
            pltpu.VMEM((units, n, own, width), bf16),
            pltpu.VMEM((units, groups, GROUP * length, length), f32),
            pltpu.VMEM((units, groups, GROUP * length, HD), bf16),
            pltpu.VMEM((units, groups, length, HD), bf16),
            pltpu.VMEM((units, groups, length, HD), bf16),
            pltpu.VMEM((2, 1, width), f32),
            pltpu.VMEM((n * reps, 2, 1, width), f32),
            dma((2, 2)),
            dma((units + 2,)),
            dma((2, units, n)),
            dma((2, units, n)),
            dma((units, n)),
            dma((units, n)),
            dma((ticks, 2)),
            dma((ticks, 2)),
            dma((4, units, reps)),
            dma((4, units, reps)),
            dma((n * reps,)),
            dma((n * reps,)),
        ],
        compiler_params=pltpu.CompilerParams(
            collective_id=0, has_side_effects=True, vmem_limit_bytes=64 * 1024 * 1024 - 65536
        ),
    )(
        normed.reshape(units, own, width),
        rows.reshape(units, own, width),
        carry_in[:, 0, 0],
        top_grad[:, 0],
        gain,
        w_qkv[:, 0],
        w_out[:, 0],
        cosine,
        sine,
        bias,
    )
    return (
        outs[0].reshape(ticks, 2, 1, 1, own, width),
        outs[1][:, None],
        outs[2][:, None],
        outs[3],
    )


def solution(mesh):
    in_specs = (
        P(None, None, "section", "dp", "tensor", None),
        P(None, "section", "dp", "tensor", None),
        P(None, "dp", "tensor", None),
        P(None, "section", None, "tensor"),
        P(None, "section", "tensor", None),
        P(None, "section", None),
    )
    out_specs = (
        P(None, None, "section", "dp", "tensor", None),
        P(None, "section", "dp", "tensor"),
        P(None, "section", ("tensor", "dp"), None),
        P(None, "section", None),
    )
    return jax.shard_map(local, mesh=mesh, in_specs=in_specs, out_specs=out_specs, check_vma=False)
```

```python
import functools
import math

import jax
import jax.numpy as jnp
from jax import lax
from jax.experimental import pallas as pl
from jax.experimental.pallas import tpu as pltpu
from jax.sharding import PartitionSpec as P

HD = 64
GROUP = 8

epsilon = 1e-06
rope_base = 1000000.0


MESH = pl.DeviceIdType.MESH

contract_rows = (((0,), (0,)), ((), ()))
contract_cols = (((1,), (1,)), ((), ()))


def from_behind(value, axis, steps):
    count = lax.axis_size(axis)
    first, last = (max(0, -steps), min(count, count - steps))
    return lax.ppermute(value, axis, [(source, source + steps) for source in range(first, last)])


def from_ahead(value, axis, steps):
    count = lax.axis_size(axis)
    return lax.ppermute(value, axis, [((i + steps) % count, i) for i in range(count)])


def rope_tables(positions, head_width):
    half_width = head_width // 2
    exponent = jnp.arange(half_width, dtype=jnp.float32) * (2.0 / head_width)
    frequency = rope_base ** (-exponent)
    angle = positions.astype(jnp.float32)[:, None] * frequency[None, :]
    return (jnp.cos(angle), jnp.sin(angle))


def rotate(values, cosine_table, sine_table, direction):
    half_width = values.shape[-1] // 2
    table_shape = (values.shape[0],) + (1,) * (values.ndim - 2) + (half_width,)
    cosine = cosine_table.reshape(table_shape)
    sine_part = direction * sine_table.reshape(table_shape)
    lower_half = values[..., :half_width]
    upper_half = values[..., half_width:]
    return jnp.concatenate(
        [
            lower_half * cosine - upper_half * sine_part,
            upper_half * cosine + lower_half * sine_part,
        ],
        axis=-1,
    )


def unit_compute(normed, grad_full, w_qkv, w_out, tables, mask):
    length = normed.shape[0]
    kv_local = w_out.shape[0] // (GROUP * HD)
    cosine_table, sine_table = tables
    score_scale = 1.0 / math.sqrt(HD)
    projected = jnp.dot(normed, w_qkv, preferred_element_type=jnp.float32)
    projected = projected.reshape(length, kv_local, GROUP + 2, HD)
    query_rot = rotate(projected[:, :, :GROUP], cosine_table, sine_table, 1.0).astype(jnp.bfloat16)
    key_rot = rotate(projected[:, :, GROUP], cosine_table, sine_table, 1.0).astype(jnp.bfloat16)
    value_rows = projected[:, :, GROUP + 1].astype(jnp.bfloat16)
    f32 = dict(preferred_element_type=jnp.float32)
    scores = jnp.einsum("tkgd,ukd->kgtu", query_rot, key_rot, **f32) * score_scale
    scores = jnp.where(mask, scores, -1e30)
    exponentials = jnp.exp(scores - jnp.max(scores, axis=-1, keepdims=True))
    softmax_rows = exponentials / jnp.sum(exponentials, axis=-1, keepdims=True)
    softmax_low = softmax_rows.astype(jnp.bfloat16)
    attended = jnp.einsum("kgtu,ukd->tkgd", softmax_low, value_rows, **f32)
    attended = attended.astype(jnp.bfloat16).reshape(length, kv_local * GROUP * HD)
    grad_attended = lax.dot_general(grad_full, w_out, contract_cols, **f32).astype(jnp.bfloat16)
    grad_heads = grad_attended.reshape(length, kv_local, GROUP, HD)
    grad_softmax = jnp.einsum("tkgd,ukd->kgtu", grad_heads, value_rows, **f32)
    row_total = jnp.sum(softmax_rows * grad_softmax, axis=-1, keepdims=True)
    grad_scores = (softmax_rows * (grad_softmax - row_total) * score_scale).astype(jnp.bfloat16)
    grad_value = jnp.einsum("kgtu,tkgd->ukd", softmax_low, grad_heads, **f32)
    grad_query = rotate(
        jnp.einsum("kgtu,ukd->tkgd", grad_scores, key_rot, **f32), cosine_table, sine_table, -1.0
    )
    grad_key = rotate(
        jnp.einsum("kgtu,tkgd->ukd", grad_scores, query_rot, **f32), cosine_table, sine_table, -1.0
    )
    grad_projected = jnp.concatenate(
        [grad_query, grad_key[:, :, None], grad_value[:, :, None]], axis=2
    )
    grad_projected = grad_projected.reshape(length, kv_local * (GROUP + 2) * HD)
    grad_projected = grad_projected.astype(jnp.bfloat16)
    partial = lax.dot_general(grad_projected, w_qkv, contract_cols, **f32).astype(jnp.bfloat16)
    return attended, grad_projected, partial


def local_permutes(layer_in, carry_in, top_grad, w_qkv, w_out, gain):
    ticks = layer_in.shape[0]
    own = layer_in.shape[4]
    n_tensor = lax.axis_size("tensor")
    n_dp = lax.axis_size("dp")
    me_tensor = lax.axis_index("tensor")
    me_dp = lax.axis_index("dp")
    section_index = lax.axis_index("section")
    at_first = section_index == 0
    at_last = section_index == lax.axis_size("section") - 1
    owners = (me_tensor + jnp.arange(n_tensor)) % n_tensor
    positions = (owners[:, None] * own + jnp.arange(own)[None, :]).reshape(-1)
    tables = rope_tables(positions, HD)
    mask = positions[:, None] >= positions[None, :]
    layer_rows = layer_in[:, :, 0, 0]
    carried = carry_in[:, 0, 0]
    fresh_grads = top_grad[:, 0]
    weight_qkv = w_qkv[:, 0]
    weight_out = w_out[:, 0]
    gain_rows = gain[:, 0]

    def gather(value):
        return jnp.concatenate(
            [value] + [from_ahead(value, "tensor", k) for k in range(1, n_tensor)], axis=0
        )

    def scatter_sum(partial):
        total = partial[:own].astype(jnp.float32)
        for k in range(1, n_tensor):
            chunk = partial[k * own : (k + 1) * own]
            total = total + from_ahead(chunk, "tensor", -k).astype(jnp.float32)
        return total

    def columns_of(value, index):
        width = value.shape[1] // n_dp
        return lax.dynamic_slice_in_dim(value, index * width, width, axis=1)

    def exchange(value, cut):
        if cut:
            return [columns_of(value, me_dp)] + [
                from_ahead(columns_of(value, (me_dp - k) % n_dp), "dp", k) for k in range(1, n_dp)
            ]
        return [value] + [from_ahead(value, "dp", k) for k in range(1, n_dp)]

    members = (1, 0)
    unit_rows, inverse, normed = {}, {}, {}
    for t in range(ticks):
        for m in members:
            rows = layer_rows[t, m].astype(jnp.float32)
            inverse[t, m] = lax.rsqrt(jnp.mean(rows * rows, axis=-1, keepdims=True) + epsilon)
            unit_rows[t, m] = rows * inverse[t, m]
            normed[t, m] = (unit_rows[t, m] * gain_rows[m]).astype(jnp.bfloat16)
    inputs = [carried[0], carried[1]]
    factors = {}
    per_tick = []
    gain_totals = [0.0, 0.0]
    for t in range(ticks):
        outcome = [None, None]
        for m in members:
            dy = inputs[m]
            full_normed = gather(normed[t, m])
            full_grad = gather(dy)
            attended, grad_projected, partial = unit_compute(
                full_normed, full_grad, weight_qkv[m], weight_out[m], tables, mask
            )
            factors[t, m] = (
                exchange(full_normed, True),
                exchange(grad_projected, False),
                exchange(attended, True),
                exchange(full_grad, False),
            )
            grad_normed = scatter_sum(partial)
            grad_unit = grad_normed * gain_rows[m]
            unit = unit_rows[t, m]
            grad_rows = inverse[t, m] * (
                grad_unit - unit * jnp.mean(grad_unit * unit, axis=-1, keepdims=True)
            )
            outcome[m] = (dy.astype(jnp.float32) + grad_rows).astype(jnp.bfloat16)
            gain_totals[m] = gain_totals[m] + jnp.sum(grad_normed * unit, axis=0)
        if t + 1 < ticks:
            upward = from_behind(outcome[1], "section", 1)
            downward = from_behind(outcome[0], "section", -1)
            inputs = [
                jnp.where(at_last, outcome[1], downward),
                jnp.where(at_first, fresh_grads[t], upward),
            ]
        per_tick.append(jnp.stack(outcome))

    def weight_grad(m, left, right):
        total = None
        for k in range(n_dp):
            a = jnp.concatenate([factors[t, m][left][k] for t in range(ticks)], axis=0)
            b = jnp.concatenate([factors[t, m][right][k] for t in range(ticks)], axis=0)
            part = lax.dot_general(a, b, contract_rows, preferred_element_type=jnp.float32)
            part = part.astype(jnp.bfloat16).astype(jnp.float32)
            total = part if total is None else total + part
        return total.astype(jnp.bfloat16)

    grad_qkv = jnp.stack([weight_grad(m, 0, 1) for m in (0, 1)])
    grad_out = jnp.stack([weight_grad(m, 2, 3) for m in (0, 1)])
    gain_total = lax.psum(jnp.stack(gain_totals), ("tensor", "dp"))
    return (
        jnp.stack(per_tick)[:, :, None, None],
        grad_qkv[:, None],
        grad_out[:, None],
        gain_total[:, None],
    )


def fused(
    n, reps, ticks, sections, own,
    nrm_own, x_ref, carry, top, gain, wq_hbm, wo_hbm, cos_ref, sin_ref, bias_ref,
    out, gq_out, go_out, gain_out,
    wq, wo, nrm, dyb, gpb, attb, pnrm, pdy, pgp, patt, pb, rb, smb, qsb, kb, vb, gtot, grecv,
    w_sem, l_sem, g_send, g_recv, r_send, r_recv, s_send, s_recv, d_send, d_recv, t_send, t_recv,
):
    f32 = jnp.float32
    bf16 = jnp.bfloat16
    me = lax.axis_index("tensor")
    rep = lax.axis_index("dp")
    sec = lax.axis_index("section")
    length = n * own
    units = 2 * ticks
    hq = wo.shape[1]
    cols = wq.shape[2]
    groups = hq // (GROUP * HD)
    wn = nrm.shape[2] // reps
    wa = hq // reps
    scale = 1.0 / math.sqrt(HD)

    def tensor_at(k):
        return {"tensor": lax.rem(me + k + n, n)}

    def dp_at(k):
        return {"dp": lax.rem(rep + k + reps, reps)}

    w_copies = [
        pltpu.make_async_copy(src.at[m], dst.at[m], w_sem.at[j, m])
        for m in (1, 0)
        for j, (src, dst) in enumerate(((wq_hbm, wq), (wo_hbm, wo)))
    ]
    for c in w_copies:
        c.start()

    barrier = pltpu.get_barrier_semaphore()
    for a in range(n):
        for b in range(reps):
            if a or b:
                pl.semaphore_signal(
                    barrier, inc=1, device_id={**tensor_at(a), **dp_at(b)}, device_id_type=MESH
                )

    @pl.when(sec > 0)
    def _():
        pl.semaphore_signal(barrier, inc=1, device_id={"section": sec - 1}, device_id_type=MESH)

    @pl.when(sec < sections - 1)
    def _():
        pl.semaphore_signal(barrier, inc=1, device_id={"section": sec + 1}, device_id_type=MESH)

    neighbours = jnp.where(sec > 0, 1, 0) + jnp.where(sec < sections - 1, 1, 0)
    with jax.named_scope("barrier"):
        pl.semaphore_wait(barrier, n * reps - 1 + neighbours)

    def remote(src, dst, send, recv, where):
        return pltpu.make_async_remote_copy(
            src_ref=src, dst_ref=dst, send_sem=send, recv_sem=recv, device_id=where,
            device_id_type=MESH,
        )

    def rows(k):
        return pl.ds(k * own, own)

    def hop(which, u, k, up):
        buf = (nrm, dyb)[which]
        there = (k - 1) % n if up else (k + 1) % n
        return remote(
            buf.at[u, rows(k)], buf.at[u, rows(there)], g_send.at[which, u, 2 * k + up],
            g_recv.at[which, u, there], tensor_at(1 if up else -1),
        )

    def arrived(which, u, k):
        at = (nrm, dyb)[which].at[u, rows(k)]
        remote(
            at, at, g_send.at[which, u, 2 * k], g_recv.at[which, u, k], tensor_at(1)
        ).wait_recv()

    def hand_on(which, u, d, act):
        @pl.when((me >= d) & (me < n - 1))
        def _():
            act(hop(which, u, (n - d) % n, 1))

        @pl.when((me + d < n) & (me > 0))
        def _():
            act(hop(which, u, d, 0))

    def gather_step(which, u, d):
        if d > 0:

            @pl.when(me >= d)
            def _():
                arrived(which, u, n - d)

            @pl.when(me + d < n)
            def _():
                arrived(which, u, d)

        if d < n - 1:
            hand_on(which, u, d, lambda c: c.start())

    def scatter_copy(u, k):
        return remote(pb.at[u, rows(k)], rb.at[u, k], r_send.at[u, k], r_recv.at[u, k], tensor_at(k))

    def dp_copy(which, u, j):
        peer = lax.rem(rep - j + reps, reps)
        nc = pl.ds(pl.multiple_of(peer * wn, 128), wn)
        ac = pl.ds(pl.multiple_of(peer * wa, 128), wa)
        src = (nrm.at[u, :, nc], dyb.at[u], gpb.at[u], attb.at[u, :, ac])[which]
        dst = (pnrm, pdy, pgp, patt)[which].at[u, j - 1]
        return remote(src, dst, d_send.at[which, u, j], d_recv.at[which, u, j], dp_at(-j))

    def section_copy(t, m):
        step = 1 if m == 1 else -1
        return remote(
            out.at[2 * t + m], dyb.at[2 * (t + 1) + m, rows(0)], s_send.at[t, m], s_recv.at[t, m],
            {"section": sec + step},
        )

    def gain_copy(a, b):
        slot = a * reps + b
        return remote(
            gtot, grecv.at[slot], t_send.at[slot], t_recv.at[slot],
            {**tensor_at(-a), **dp_at(-b)},
        )

    peers = range(1, n)
    others = range(1, reps)

    local_copies = []
    for u in range(units):
        local_copies.append(pltpu.make_async_copy(nrm_own.at[u], nrm.at[u, rows(0)], l_sem.at[u]))
    for m in (0, 1):
        local_copies.append(
            pltpu.make_async_copy(carry.at[m], dyb.at[m, rows(0)], l_sem.at[units + m])
        )
    for c in local_copies:
        c.start()
    for c in local_copies:
        c.wait()
    for which in (0, 1):
        gather_step(which, 1, 0)
    gtot[...] = jnp.zeros_like(gtot)
    with jax.named_scope("wait_weights"):
        for c in w_copies:
            c.wait()

    def swap(values):
        width = values.shape[1]
        lane = lax.broadcasted_iota(jnp.int32, values.shape, 1)
        low = lax.rem(lane, HD) < HD // 2
        return jnp.where(
            low, pltpu.roll(values, width - HD // 2, 1), pltpu.roll(values, HD // 2, 1)
        )

    def dot(a, b, ca, cb):
        return lax.dot_general(a, b, (((ca,), (cb,)), ((), ())), preferred_element_type=f32)

    def stack_heads(values):
        return jnp.concatenate([values[:, h * HD : (h + 1) * HD] for h in range(GROUP)], axis=0)

    def spread_heads(values):
        return jnp.concatenate(
            [values[h * length : (h + 1) * length] for h in range(GROUP)], axis=1
        )

    span = (GROUP + 2) * HD

    def forward(u, m):
        for j in others:
            dp_copy(0, u, j).start()
        projected = dot(nrm[u], wq[m], 1, 0)
        rotated = (projected * cos_ref[...] + swap(projected) * sin_ref[...]).astype(bf16)
        for g in range(groups):
            at = g * span
            qs = stack_heads(rotated[:, at : at + GROUP * HD])
            key = rotated[:, at + GROUP * HD : at + (GROUP + 1) * HD]
            value = projected[:, at + (GROUP + 1) * HD : at + span].astype(bf16)
            scores = dot(qs, key, 1, 1) * scale
            scores = (scores.reshape(GROUP, length, length) + bias_ref[...][None]).reshape(
                GROUP * length, length
            )
            e = jnp.exp(scores - jnp.max(scores, axis=-1, keepdims=True))
            sm = e / jnp.sum(e, axis=-1, keepdims=True)
            smb[u, g] = sm
            qsb[u, g] = qs
            kb[u, g] = key
            vb[u, g] = value
            attended = spread_heads(dot(sm.astype(bf16), value, 1, 0).astype(bf16))
            attb[u, :, g * GROUP * HD : (g + 1) * GROUP * HD] = attended
        for j in others:
            dp_copy(3, u, j).start()

    def backward(u, m):
        for j in others:
            dp_copy(1, u, j).start()
        grad_att = dot(dyb[u], wo[m], 1, 1).astype(bf16)
        for g in range(groups):
            sm = smb[u, g]
            low = sm.astype(bf16)
            value = vb[u, g]
            gs = stack_heads(grad_att[:, g * GROUP * HD : (g + 1) * GROUP * HD])
            gsm = dot(gs, value, 1, 1)
            total = jnp.sum(sm * gsm, axis=-1, keepdims=True)
            gsc = (sm * (gsm - total) * scale).astype(bf16)
            g_value = dot(low, gs, 0, 0)
            g_query = spread_heads(dot(gsc, kb[u, g], 1, 0))
            g_key = dot(gsc, qsb[u, g], 0, 0)
            turned = jnp.concatenate([g_query, g_key, g_value], axis=1)
            cs = cos_ref[:, g * span : (g + 1) * span]
            sn = sin_ref[:, g * span : (g + 1) * span]
            back = turned * cs - swap(turned) * sn
            lane = lax.broadcasted_iota(jnp.int32, turned.shape, 1)
            back = jnp.where(lane < (GROUP + 1) * HD, back, turned)
            gpb[u, :, g * span : (g + 1) * span] = back.astype(bf16)
        for j in others:
            dp_copy(2, u, j).start()
        pb[u] = dot(gpb[u], wq[m], 1, 1).astype(bf16)
        for k in peers:
            scatter_copy(u, k).start()

    def finish(u, m):
        x = x_ref[u].astype(f32)
        inverse = lax.rsqrt(jnp.mean(x * x, axis=-1, keepdims=True) + epsilon)
        unit = x * inverse
        gn = pb[u, 0:own].astype(f32)
        with jax.named_scope("wait_scatter"):
            for k in peers:
                scatter_copy(u, k).wait_recv()
        for k in peers:
            gn = gn + rb[u, k].astype(f32)
        gu = gn * gain[m]
        grad = inverse * (gu - unit * jnp.mean(gu * unit, axis=-1, keepdims=True))
        out[u] = (dyb[u, 0:own].astype(f32) + grad).astype(bf16)
        gtot[m] = gtot[m] + jnp.sum(gn * unit, axis=0, keepdims=True)

    def weight_grads(m):
        def part(a_of, b_of):
            p = None
            for t in range(ticks):
                q = dot(a_of(2 * t + m), b_of(2 * t + m), 0, 0)
                p = q if p is None else p + q
            return p.astype(bf16).astype(f32)

        block = 256 if wn % 256 == 0 else 128

        @pl.loop(0, wn // block)
        def _(c):
            own_at = pl.ds(pl.multiple_of(rep * wn + c * block, 128), block)
            at = pl.ds(pl.multiple_of(c * block, 128), block)
            total = part(lambda u: nrm[u, :, own_at], lambda u: gpb[u])
            for j in others:
                total = total + part(lambda u: pnrm[u, j - 1, :, at], lambda u: pgp[u, j - 1])
            gq_out[m, at] = total.astype(bf16)

        width = dyb.shape[2]
        wide = 512 if width % 512 == 0 else 128
        att_at = pl.ds(pl.multiple_of(rep * wa, 128), wa)

        @pl.loop(0, width // wide)
        def _(c):
            at = pl.ds(pl.multiple_of(c * wide, 128), wide)
            total = part(lambda u: attb[u, :, att_at], lambda u: dyb[u, :, at])
            for j in others:
                total = total + part(lambda u: patt[u, j - 1], lambda u: pdy[u, j - 1, :, at])
            go_out[m, :, at] = total.astype(bf16)

    def steps(pairs):
        for which, u, d in pairs:
            with jax.named_scope("gather_step"):
                gather_step(which, u, d)

    def both(u, *ds):
        return [(which, u, d) for d in ds for which in (0, 1)]

    far = range(1, n)
    steps(both(1, 1))
    steps(both(0, 0))
    steps(both(1, *far[1:-1]))
    steps(both(0, 1))
    steps([(0, 1, n - 1)])
    with jax.named_scope("forward"):
        forward(1, 1)
    steps([(1, 1, n - 1)])
    with jax.named_scope("backward"):
        backward(1, 1)
    steps(both(0, *far[1:]))
    with jax.named_scope("forward"):
        forward(0, 0)
    with jax.named_scope("backward"):
        backward(0, 0)
    for t in range(ticks - 1):
        here, there = 2 * t, 2 * (t + 1)
        for d in range(2):
            steps([(0, there + 1, d), (0, there, d)])
        finish(here + 1, 1)

        @pl.when(sec < sections - 1)
        def _():
            section_copy(t, 1).start()

        @pl.when(sec == sections - 1)
        def _():
            dyb[there, 0:own] = out[here + 1]

        @pl.when(sec == 0)
        def _():
            dyb[there + 1, 0:own] = top[t]

        for d in far[1:-1]:
            steps([(0, there + 1, d), (0, there, d)])
        finish(here, 0)

        @pl.when(sec > 0)
        def _():
            section_copy(t, 0).start()

        for m in (1, 0):
            steps([(0, there + m, n - 1)])
            with jax.named_scope("forward"):
                forward(there + m, m)

        @pl.when(sec > 0)
        def _():
            with jax.named_scope("wait_section"):
                section_copy(t, 1).wait_recv()

        steps([(1, there + 1, 0)])

        @pl.when(sec < sections - 1)
        def _():
            with jax.named_scope("wait_section"):
                section_copy(t, 0).wait_recv()

        steps([(1, there, 0)])
        for d in far[:-1]:
            steps([(1, there + 1, d), (1, there, d)])
        for m in (1, 0):
            steps([(1, there + m, n - 1)])
            with jax.named_scope("backward"):
                backward(there + m, m)

    last = 2 * (ticks - 1)
    for m in (1, 0):
        finish(last + m, m)
    for a in range(n):
        for b in range(reps):
            if a or b:
                gain_copy(a, b).start()
    for m in (1, 0):
        with jax.named_scope("wait_dp"):
            for t in range(ticks):
                for which in range(4):
                    for j in others:
                        dp_copy(which, 2 * t + m, j).wait_recv()
        with jax.named_scope("weight_grads"):
            weight_grads(m)
    total = gtot[...]
    for a in range(n):
        for b in range(reps):
            if a or b:
                gain_copy(a, b).wait_recv()
                total = total + grecv[a * reps + b]
    gain_out[...] = total
    for u in range(units):
        for k in peers:
            scatter_copy(u, k).wait_send()
        for d in range(n - 1):
            for which in (0, 1):
                hand_on(which, u, d, lambda c: c.wait_send())
        for j in others:
            for which in range(4):
                dp_copy(which, u, j).wait_send()
    for t in range(ticks - 1):

        @pl.when(sec < sections - 1)
        def _():
            section_copy(t, 1).wait_send()

        @pl.when(sec > 0)
        def _():
            section_copy(t, 0).wait_send()

    for a in range(n):
        for b in range(reps):
            if a or b:
                gain_copy(a, b).wait_send()


def local(layer_in, carry_in, top_grad, w_qkv, w_out, gain):
    ticks, own, width = layer_in.shape[0], layer_in.shape[4], layer_in.shape[5]
    n = lax.axis_size("tensor")
    reps = lax.axis_size("dp")
    sections = lax.axis_size("section")
    cols, hq = w_qkv.shape[3], w_out.shape[2]
    if (width // reps) % 128 or (hq // reps) % 128 or ticks < 2:
        return local_permutes(layer_in, carry_in, top_grad, w_qkv, w_out, gain)
    length = n * own
    units = 2 * ticks
    groups = hq // (GROUP * HD)
    wn, wa = width // reps, hq // reps
    f32, bf16 = jnp.float32, jnp.bfloat16
    me = lax.axis_index("tensor")
    owners = (me + jnp.arange(n)) % n
    positions = (owners[:, None] * own + jnp.arange(own)[None, :]).reshape(-1)
    cosine, sine = rope_tables(positions, HD)
    slots = cols // HD
    cosine = jnp.tile(jnp.concatenate([cosine, cosine], axis=1), (1, slots))
    sine = jnp.tile(jnp.concatenate([-sine, sine], axis=1), (1, slots))
    bias = jnp.where(positions[:, None] >= positions[None, :], 0.0, -1e30).astype(f32)
    rows = layer_in[:, :, 0, 0]
    wide = rows.astype(f32)
    inverse = lax.rsqrt(jnp.mean(wide * wide, axis=-1, keepdims=True) + epsilon)
    normed = (wide * inverse * gain[:, 0][None, :, None, :]).astype(bf16)
    vmem = pl.BlockSpec(memory_space=pltpu.VMEM)
    hbm = pl.BlockSpec(memory_space=pl.ANY)
    dma = pltpu.SemaphoreType.DMA
    outs = pl.pallas_call(
        functools.partial(fused, n, reps, ticks, sections, own),
        out_shape=(
            jax.ShapeDtypeStruct((units, own, width), bf16),
            jax.ShapeDtypeStruct((2, wn, cols), bf16),
            jax.ShapeDtypeStruct((2, wa, width), bf16),
            jax.ShapeDtypeStruct((2, 1, width), f32),
        ),
        in_specs=[vmem] * 5 + [hbm] * 2 + [vmem] * 3,
        out_specs=(vmem,) * 4,
        scratch_shapes=[
            pltpu.VMEM((2, width, cols), bf16),
            pltpu.VMEM((2, hq, width), bf16),
            pltpu.VMEM((units, length, width), bf16),
            pltpu.VMEM((units, length, width), bf16),
            pltpu.VMEM((units, length, cols), bf16),
            pltpu.VMEM((units, length, hq), bf16),
            pltpu.VMEM((units, reps - 1, length, wn), bf16),
            pltpu.VMEM((units, reps - 1, length, width), bf16),
            pltpu.VMEM((units, reps - 1, length, cols), bf16),
            pltpu.VMEM((units, reps - 1, length, wa), bf16),
            pltpu.VMEM((units, length, width), bf16),
            pltpu.VMEM((units, n, own, width), bf16),
            pltpu.VMEM((units, groups, GROUP * length, length), f32),
            pltpu.VMEM((units, groups, GROUP * length, HD), bf16),
            pltpu.VMEM((units, groups, length, HD), bf16),
            pltpu.VMEM((units, groups, length, HD), bf16),
            pltpu.VMEM((2, 1, width), f32),
            pltpu.VMEM((n * reps, 2, 1, width), f32),
            dma((2, 2)),
            dma((units + 2,)),
            dma((2, units, 2 * n)),
            dma((2, units, n)),
            dma((units, n)),
            dma((units, n)),
            dma((ticks, 2)),
            dma((ticks, 2)),
            dma((4, units, reps)),
            dma((4, units, reps)),
            dma((n * reps,)),
            dma((n * reps,)),
        ],
        compiler_params=pltpu.CompilerParams(
            collective_id=0, has_side_effects=True, vmem_limit_bytes=64 * 1024 * 1024 - 65536
        ),
    )(
        normed.reshape(units, own, width),
        rows.reshape(units, own, width),
        carry_in[:, 0, 0],
        top_grad[:, 0],
        gain,
        w_qkv[:, 0],
        w_out[:, 0],
        cosine,
        sine,
        bias,
    )
    return (
        outs[0].reshape(ticks, 2, 1, 1, own, width),
        outs[1][:, None],
        outs[2][:, None],
        outs[3],
    )


def solution(mesh):
    in_specs = (
        P(None, None, "section", "dp", "tensor", None),
        P(None, "section", "dp", "tensor", None),
        P(None, "dp", "tensor", None),
        P(None, "section", None, "tensor"),
        P(None, "section", "tensor", None),
        P(None, "section", None),
    )
    out_specs = (
        P(None, None, "section", "dp", "tensor", None),
        P(None, "section", "dp", "tensor"),
        P(None, "section", ("tensor", "dp"), None),
        P(None, "section", None),
    )
    return jax.shard_map(local, mesh=mesh, in_specs=in_specs, out_specs=out_specs, check_vma=False)
```

```python
import functools
import math

import jax
import jax.numpy as jnp
from jax import lax
from jax.experimental import pallas as pl
from jax.experimental.pallas import tpu as pltpu
from jax.sharding import PartitionSpec as P

HD = 64
GROUP = 8

epsilon = 1e-06
rope_base = 1000000.0


MESH = pl.DeviceIdType.MESH

contract_rows = (((0,), (0,)), ((), ()))
contract_cols = (((1,), (1,)), ((), ()))


def from_behind(value, axis, steps):
    count = lax.axis_size(axis)
    first, last = (max(0, -steps), min(count, count - steps))
    return lax.ppermute(value, axis, [(source, source + steps) for source in range(first, last)])


def from_ahead(value, axis, steps):
    count = lax.axis_size(axis)
    return lax.ppermute(value, axis, [((i + steps) % count, i) for i in range(count)])


def rope_tables(positions, head_width):
    half_width = head_width // 2
    exponent = jnp.arange(half_width, dtype=jnp.float32) * (2.0 / head_width)
    frequency = rope_base ** (-exponent)
    angle = positions.astype(jnp.float32)[:, None] * frequency[None, :]
    return (jnp.cos(angle), jnp.sin(angle))


def rotate(values, cosine_table, sine_table, direction):
    half_width = values.shape[-1] // 2
    table_shape = (values.shape[0],) + (1,) * (values.ndim - 2) + (half_width,)
    cosine = cosine_table.reshape(table_shape)
    sine_part = direction * sine_table.reshape(table_shape)
    lower_half = values[..., :half_width]
    upper_half = values[..., half_width:]
    return jnp.concatenate(
        [
            lower_half * cosine - upper_half * sine_part,
            upper_half * cosine + lower_half * sine_part,
        ],
        axis=-1,
    )


def unit_compute(normed, grad_full, w_qkv, w_out, tables, mask):
    length = normed.shape[0]
    kv_local = w_out.shape[0] // (GROUP * HD)
    cosine_table, sine_table = tables
    score_scale = 1.0 / math.sqrt(HD)
    projected = jnp.dot(normed, w_qkv, preferred_element_type=jnp.float32)
    projected = projected.reshape(length, kv_local, GROUP + 2, HD)
    query_rot = rotate(projected[:, :, :GROUP], cosine_table, sine_table, 1.0).astype(jnp.bfloat16)
    key_rot = rotate(projected[:, :, GROUP], cosine_table, sine_table, 1.0).astype(jnp.bfloat16)
    value_rows = projected[:, :, GROUP + 1].astype(jnp.bfloat16)
    f32 = dict(preferred_element_type=jnp.float32)
    scores = jnp.einsum("tkgd,ukd->kgtu", query_rot, key_rot, **f32) * score_scale
    scores = jnp.where(mask, scores, -1e30)
    exponentials = jnp.exp(scores - jnp.max(scores, axis=-1, keepdims=True))
    softmax_rows = exponentials / jnp.sum(exponentials, axis=-1, keepdims=True)
    softmax_low = softmax_rows.astype(jnp.bfloat16)
    attended = jnp.einsum("kgtu,ukd->tkgd", softmax_low, value_rows, **f32)
    attended = attended.astype(jnp.bfloat16).reshape(length, kv_local * GROUP * HD)
    grad_attended = lax.dot_general(grad_full, w_out, contract_cols, **f32).astype(jnp.bfloat16)
    grad_heads = grad_attended.reshape(length, kv_local, GROUP, HD)
    grad_softmax = jnp.einsum("tkgd,ukd->kgtu", grad_heads, value_rows, **f32)
    row_total = jnp.sum(softmax_rows * grad_softmax, axis=-1, keepdims=True)
    grad_scores = (softmax_rows * (grad_softmax - row_total) * score_scale).astype(jnp.bfloat16)
    grad_value = jnp.einsum("kgtu,tkgd->ukd", softmax_low, grad_heads, **f32)
    grad_query = rotate(
        jnp.einsum("kgtu,ukd->tkgd", grad_scores, key_rot, **f32), cosine_table, sine_table, -1.0
    )
    grad_key = rotate(
        jnp.einsum("kgtu,tkgd->ukd", grad_scores, query_rot, **f32), cosine_table, sine_table, -1.0
    )
    grad_projected = jnp.concatenate(
        [grad_query, grad_key[:, :, None], grad_value[:, :, None]], axis=2
    )
    grad_projected = grad_projected.reshape(length, kv_local * (GROUP + 2) * HD)
    grad_projected = grad_projected.astype(jnp.bfloat16)
    partial = lax.dot_general(grad_projected, w_qkv, contract_cols, **f32).astype(jnp.bfloat16)
    return attended, grad_projected, partial


def local_permutes(layer_in, carry_in, top_grad, w_qkv, w_out, gain):
    ticks = layer_in.shape[0]
    own = layer_in.shape[4]
    n_tensor = lax.axis_size("tensor")
    n_dp = lax.axis_size("dp")
    me_tensor = lax.axis_index("tensor")
    me_dp = lax.axis_index("dp")
    section_index = lax.axis_index("section")
    at_first = section_index == 0
    at_last = section_index == lax.axis_size("section") - 1
    owners = (me_tensor + jnp.arange(n_tensor)) % n_tensor
    positions = (owners[:, None] * own + jnp.arange(own)[None, :]).reshape(-1)
    tables = rope_tables(positions, HD)
    mask = positions[:, None] >= positions[None, :]
    layer_rows = layer_in[:, :, 0, 0]
    carried = carry_in[:, 0, 0]
    fresh_grads = top_grad[:, 0]
    weight_qkv = w_qkv[:, 0]
    weight_out = w_out[:, 0]
    gain_rows = gain[:, 0]

    def gather(value):
        return jnp.concatenate(
            [value] + [from_ahead(value, "tensor", k) for k in range(1, n_tensor)], axis=0
        )

    def scatter_sum(partial):
        total = partial[:own].astype(jnp.float32)
        for k in range(1, n_tensor):
            chunk = partial[k * own : (k + 1) * own]
            total = total + from_ahead(chunk, "tensor", -k).astype(jnp.float32)
        return total

    def columns_of(value, index):
        width = value.shape[1] // n_dp
        return lax.dynamic_slice_in_dim(value, index * width, width, axis=1)

    def exchange(value, cut):
        if cut:
            return [columns_of(value, me_dp)] + [
                from_ahead(columns_of(value, (me_dp - k) % n_dp), "dp", k) for k in range(1, n_dp)
            ]
        return [value] + [from_ahead(value, "dp", k) for k in range(1, n_dp)]

    members = (1, 0)
    unit_rows, inverse, normed = {}, {}, {}
    for t in range(ticks):
        for m in members:
            rows = layer_rows[t, m].astype(jnp.float32)
            inverse[t, m] = lax.rsqrt(jnp.mean(rows * rows, axis=-1, keepdims=True) + epsilon)
            unit_rows[t, m] = rows * inverse[t, m]
            normed[t, m] = (unit_rows[t, m] * gain_rows[m]).astype(jnp.bfloat16)
    inputs = [carried[0], carried[1]]
    factors = {}
    per_tick = []
    gain_totals = [0.0, 0.0]
    for t in range(ticks):
        outcome = [None, None]
        for m in members:
            dy = inputs[m]
            full_normed = gather(normed[t, m])
            full_grad = gather(dy)
            attended, grad_projected, partial = unit_compute(
                full_normed, full_grad, weight_qkv[m], weight_out[m], tables, mask
            )
            factors[t, m] = (
                exchange(full_normed, True),
                exchange(grad_projected, False),
                exchange(attended, True),
                exchange(full_grad, False),
            )
            grad_normed = scatter_sum(partial)
            grad_unit = grad_normed * gain_rows[m]
            unit = unit_rows[t, m]
            grad_rows = inverse[t, m] * (
                grad_unit - unit * jnp.mean(grad_unit * unit, axis=-1, keepdims=True)
            )
            outcome[m] = (dy.astype(jnp.float32) + grad_rows).astype(jnp.bfloat16)
            gain_totals[m] = gain_totals[m] + jnp.sum(grad_normed * unit, axis=0)
        if t + 1 < ticks:
            upward = from_behind(outcome[1], "section", 1)
            downward = from_behind(outcome[0], "section", -1)
            inputs = [
                jnp.where(at_last, outcome[1], downward),
                jnp.where(at_first, fresh_grads[t], upward),
            ]
        per_tick.append(jnp.stack(outcome))

    def weight_grad(m, left, right):
        total = None
        for k in range(n_dp):
            a = jnp.concatenate([factors[t, m][left][k] for t in range(ticks)], axis=0)
            b = jnp.concatenate([factors[t, m][right][k] for t in range(ticks)], axis=0)
            part = lax.dot_general(a, b, contract_rows, preferred_element_type=jnp.float32)
            part = part.astype(jnp.bfloat16).astype(jnp.float32)
            total = part if total is None else total + part
        return total.astype(jnp.bfloat16)

    grad_qkv = jnp.stack([weight_grad(m, 0, 1) for m in (0, 1)])
    grad_out = jnp.stack([weight_grad(m, 2, 3) for m in (0, 1)])
    gain_total = lax.psum(jnp.stack(gain_totals), ("tensor", "dp"))
    return (
        jnp.stack(per_tick)[:, :, None, None],
        grad_qkv[:, None],
        grad_out[:, None],
        gain_total[:, None],
    )


def fused(
    n, reps, ticks, sections, own,
    nrm_own, x_ref, carry, top, gain, wq_hbm, wo_hbm, cos_ref, sin_ref, bias_ref,
    out, gq_out, go_out, gain_out,
    wq, wo, nrm, dyb, gpb, attb, pnrm, pdy, pgp, patt, pb, rb, smb, qsb, kb, vb, gtot, grecv, gsum,
    w_sem, l_sem, g_send, g_recv, r_send, r_recv, s_send, s_recv, d_send, d_recv, t_send, t_recv,
):
    f32 = jnp.float32
    bf16 = jnp.bfloat16
    me = lax.axis_index("tensor")
    rep = lax.axis_index("dp")
    sec = lax.axis_index("section")
    length = n * own
    units = 2 * ticks
    hq = wo.shape[1]
    cols = wq.shape[2]
    groups = hq // (GROUP * HD)
    wn = nrm.shape[2] // reps
    wa = hq // reps
    scale = 1.0 / math.sqrt(HD)

    def tensor_at(k):
        return {"tensor": lax.rem(me + k + n, n)}

    def dp_at(k):
        return {"dp": lax.rem(rep + k + reps, reps)}

    w_copies = [
        pltpu.make_async_copy(src.at[m], dst.at[m], w_sem.at[j, m])
        for m in (1, 0)
        for j, (src, dst) in enumerate(((wq_hbm, wq), (wo_hbm, wo)))
    ]
    for c in w_copies:
        c.start()

    barrier = pltpu.get_barrier_semaphore()
    for a in range(n):
        for b in range(reps):
            if a or b:
                pl.semaphore_signal(
                    barrier, inc=1, device_id={**tensor_at(a), **dp_at(b)}, device_id_type=MESH
                )

    @pl.when(sec > 0)
    def _():
        pl.semaphore_signal(barrier, inc=1, device_id={"section": sec - 1}, device_id_type=MESH)

    @pl.when(sec < sections - 1)
    def _():
        pl.semaphore_signal(barrier, inc=1, device_id={"section": sec + 1}, device_id_type=MESH)

    neighbours = jnp.where(sec > 0, 1, 0) + jnp.where(sec < sections - 1, 1, 0)
    with jax.named_scope("barrier"):
        pl.semaphore_wait(barrier, n * reps - 1 + neighbours)

    def remote(src, dst, send, recv, where):
        return pltpu.make_async_remote_copy(
            src_ref=src, dst_ref=dst, send_sem=send, recv_sem=recv, device_id=where,
            device_id_type=MESH,
        )

    def rows(k):
        return pl.ds(k * own, own)

    def hop(which, u, k, up):
        buf = (nrm, dyb)[which]
        there = (k - 1) % n if up else (k + 1) % n
        return remote(
            buf.at[u, rows(k)], buf.at[u, rows(there)], g_send.at[which, u, 2 * k + up],
            g_recv.at[which, u, there], tensor_at(1 if up else -1),
        )

    def arrived(which, u, k):
        at = (nrm, dyb)[which].at[u, rows(k)]
        remote(
            at, at, g_send.at[which, u, 2 * k], g_recv.at[which, u, k], tensor_at(1)
        ).wait_recv()

    def hand_on(which, u, d, act):
        @pl.when((me >= d) & (me < n - 1))
        def _():
            act(hop(which, u, (n - d) % n, 1))

        @pl.when((me + d < n) & (me > 0))
        def _():
            act(hop(which, u, d, 0))

    def gather_step(which, u, d):
        if d > 0:

            @pl.when(me >= d)
            def _():
                arrived(which, u, n - d)

            @pl.when(me + d < n)
            def _():
                arrived(which, u, d)

        if d < n - 1:
            hand_on(which, u, d, lambda c: c.start())

    def sum_copy(u, d, way):
        k = d if way else n - d
        return remote(
            pb.at[u, rows(k)], rb.at[u, way, d - 1], r_send.at[u, way, d],
            r_recv.at[u, way, d - 1], tensor_at(1 if way else -1),
        )

    def sum_arrived(u, d, way):
        at = rb.at[u, way, d]
        remote(
            at, at, r_send.at[u, way, d], r_recv.at[u, way, d], tensor_at(1)
        ).wait_recv()

    def scatter_step(u, stage):
        for way in (1, 0):

            @pl.when(me == (stage if way else n - 1 - stage))
            def _():
                for d in range(n - 1 - stage, 0, -1):
                    if stage:
                        at = rows(d if way else n - d)
                        sum_arrived(u, d, way)
                        total = pb[u, at].astype(f32) + rb[u, way, d].astype(f32)
                        pb[u, at] = total.astype(bf16)
                    sum_copy(u, d, way).start()

    def sums_sent(u):
        for way in (1, 0):
            for stage in range(n - 1):

                @pl.when(me == (stage if way else n - 1 - stage))
                def _():
                    for d in range(n - 1 - stage, 0, -1):
                        sum_copy(u, d, way).wait_send()

    def dp_copy(which, u, j):
        peer = lax.rem(rep - j + reps, reps)
        nc = pl.ds(pl.multiple_of(peer * wn, 128), wn)
        ac = pl.ds(pl.multiple_of(peer * wa, 128), wa)
        src = (nrm.at[u, :, nc], dyb.at[u], gpb.at[u], attb.at[u, :, ac])[which]
        dst = (pnrm, pdy, pgp, patt)[which].at[u, j - 1]
        return remote(src, dst, d_send.at[which, u, j], d_recv.at[which, u, j], dp_at(-j))

    def section_copy(t, m):
        step = 1 if m == 1 else -1
        return remote(
            out.at[2 * t + m], dyb.at[2 * (t + 1) + m, rows(0)], s_send.at[t, m], s_recv.at[t, m],
            {"section": sec + step},
        )

    def gain_copy(a, b):
        slot = a * reps + b
        return remote(
            gtot, grecv.at[slot], t_send.at[slot], t_recv.at[slot],
            {**tensor_at(-a), **dp_at(-b)},
        )

    peers = range(1, n)
    others = range(1, reps)

    local_copies = []
    for u in range(units):
        local_copies.append(pltpu.make_async_copy(nrm_own.at[u], nrm.at[u, rows(0)], l_sem.at[u]))
    for m in (0, 1):
        local_copies.append(
            pltpu.make_async_copy(carry.at[m], dyb.at[m, rows(0)], l_sem.at[units + m])
        )
    for c in local_copies:
        c.start()
    for c in local_copies:
        c.wait()
    for which in (0, 1):
        gather_step(which, 1, 0)
    gtot[...] = jnp.zeros_like(gtot)
    with jax.named_scope("wait_weights"):
        for c in w_copies:
            c.wait()

    def swap(values):
        width = values.shape[1]
        lane = lax.broadcasted_iota(jnp.int32, values.shape, 1)
        low = lax.rem(lane, HD) < HD // 2
        return jnp.where(
            low, pltpu.roll(values, width - HD // 2, 1), pltpu.roll(values, HD // 2, 1)
        )

    def dot(a, b, ca, cb):
        return lax.dot_general(a, b, (((ca,), (cb,)), ((), ())), preferred_element_type=f32)

    def stack_heads(values):
        return jnp.concatenate([values[:, h * HD : (h + 1) * HD] for h in range(GROUP)], axis=0)

    def spread_heads(values):
        return jnp.concatenate(
            [values[h * length : (h + 1) * length] for h in range(GROUP)], axis=1
        )

    span = (GROUP + 2) * HD

    def forward(u, m):
        for j in others:
            dp_copy(0, u, j).start()
        projected = dot(nrm[u], wq[m], 1, 0)
        rotated = (projected * cos_ref[...] + swap(projected) * sin_ref[...]).astype(bf16)
        for g in range(groups):
            at = g * span
            qs = stack_heads(rotated[:, at : at + GROUP * HD])
            key = rotated[:, at + GROUP * HD : at + (GROUP + 1) * HD]
            value = projected[:, at + (GROUP + 1) * HD : at + span].astype(bf16)
            scores = dot(qs, key, 1, 1) * scale
            scores = (scores.reshape(GROUP, length, length) + bias_ref[...][None]).reshape(
                GROUP * length, length
            )
            e = jnp.exp(scores - jnp.max(scores, axis=-1, keepdims=True))
            sm = e / jnp.sum(e, axis=-1, keepdims=True)
            smb[u, g] = sm
            qsb[u, g] = qs
            kb[u, g] = key
            vb[u, g] = value
            attended = spread_heads(dot(sm.astype(bf16), value, 1, 0).astype(bf16))
            attb[u, :, g * GROUP * HD : (g + 1) * GROUP * HD] = attended
        for j in others:
            dp_copy(3, u, j).start()

    def backward(u, m):
        for j in others:
            dp_copy(1, u, j).start()
        grad_att = dot(dyb[u], wo[m], 1, 1).astype(bf16)
        for g in range(groups):
            sm = smb[u, g]
            low = sm.astype(bf16)
            value = vb[u, g]
            gs = stack_heads(grad_att[:, g * GROUP * HD : (g + 1) * GROUP * HD])
            gsm = dot(gs, value, 1, 1)
            total = jnp.sum(sm * gsm, axis=-1, keepdims=True)
            gsc = (sm * (gsm - total) * scale).astype(bf16)
            g_value = dot(low, gs, 0, 0)
            g_query = spread_heads(dot(gsc, kb[u, g], 1, 0))
            g_key = dot(gsc, qsb[u, g], 0, 0)
            turned = jnp.concatenate([g_query, g_key, g_value], axis=1)
            cs = cos_ref[:, g * span : (g + 1) * span]
            sn = sin_ref[:, g * span : (g + 1) * span]
            back = turned * cs - swap(turned) * sn
            lane = lax.broadcasted_iota(jnp.int32, turned.shape, 1)
            back = jnp.where(lane < (GROUP + 1) * HD, back, turned)
            gpb[u, :, g * span : (g + 1) * span] = back.astype(bf16)
        for j in others:
            dp_copy(2, u, j).start()
        pb[u] = dot(gpb[u], wq[m], 1, 1).astype(bf16)
        scatter_step(u, 0)

    def finish(u, m):
        x = x_ref[u].astype(f32)
        inverse = lax.rsqrt(jnp.mean(x * x, axis=-1, keepdims=True) + epsilon)
        unit = x * inverse
        gsum[...] = pb[u, 0:own].astype(f32)
        with jax.named_scope("wait_scatter"):
            for way in (1, 0):

                @pl.when(me > 0 if way else me < n - 1)
                def _():
                    sum_arrived(u, 0, way)
                    gsum[...] = gsum[...] + rb[u, way, 0].astype(f32)

        gn = gsum[...]
        gu = gn * gain[m]
        grad = inverse * (gu - unit * jnp.mean(gu * unit, axis=-1, keepdims=True))
        out[u] = (dyb[u, 0:own].astype(f32) + grad).astype(bf16)
        gtot[m] = gtot[m] + jnp.sum(gn * unit, axis=0, keepdims=True)

    def weight_grads(m):
        def part(a_of, b_of):
            p = None
            for t in range(ticks):
                q = dot(a_of(2 * t + m), b_of(2 * t + m), 0, 0)
                p = q if p is None else p + q
            return p.astype(bf16).astype(f32)

        block = 256 if wn % 256 == 0 else 128

        @pl.loop(0, wn // block)
        def _(c):
            own_at = pl.ds(pl.multiple_of(rep * wn + c * block, 128), block)
            at = pl.ds(pl.multiple_of(c * block, 128), block)
            total = part(lambda u: nrm[u, :, own_at], lambda u: gpb[u])
            for j in others:
                total = total + part(lambda u: pnrm[u, j - 1, :, at], lambda u: pgp[u, j - 1])
            gq_out[m, at] = total.astype(bf16)

        width = dyb.shape[2]
        wide = 512 if width % 512 == 0 else 128
        att_at = pl.ds(pl.multiple_of(rep * wa, 128), wa)

        @pl.loop(0, width // wide)
        def _(c):
            at = pl.ds(pl.multiple_of(c * wide, 128), wide)
            total = part(lambda u: attb[u, :, att_at], lambda u: dyb[u, :, at])
            for j in others:
                total = total + part(lambda u: patt[u, j - 1], lambda u: pdy[u, j - 1, :, at])
            go_out[m, :, at] = total.astype(bf16)

    def steps(pairs):
        for which, u, d in pairs:
            with jax.named_scope("gather_step"):
                gather_step(which, u, d)

    def both(u, *ds):
        return [(which, u, d) for d in ds for which in (0, 1)]

    def sums(u, *stages):
        for stage in stages:
            with jax.named_scope("scatter_step"):
                scatter_step(u, stage)

    far = range(1, n)
    steps(both(1, 1))
    steps(both(0, 0))
    steps(both(1, *far[1:-1]))
    steps(both(0, 1))
    steps([(0, 1, n - 1)])
    with jax.named_scope("forward"):
        forward(1, 1)
    steps([(1, 1, n - 1)])
    with jax.named_scope("backward"):
        backward(1, 1)
    steps(both(0, *far[1:-1]))
    sums(1, *far[:-2])
    steps([(0, 0, n - 1)])
    with jax.named_scope("forward"):
        forward(0, 0)
    steps([(1, 0, n - 1)])
    with jax.named_scope("backward"):
        backward(0, 0)
    sums(1, *far[-2:-1])
    for t in range(ticks - 1):
        here, there = 2 * t, 2 * (t + 1)
        if t > 0:
            sums(here + 1, *far[:-1])
        steps([(0, there + 1, 0), (0, there, 0)])
        finish(here + 1, 1)

        @pl.when(sec < sections - 1)
        def _():
            section_copy(t, 1).start()

        @pl.when(sec == sections - 1)
        def _():
            dyb[there, 0:own] = out[here + 1]

        @pl.when(sec == 0)
        def _():
            dyb[there + 1, 0:own] = top[t]

        for stage in far[:-1]:
            sums(here, stage)
            steps([(0, there + 1, stage), (0, there, stage)])
        finish(here, 0)

        @pl.when(sec > 0)
        def _():
            section_copy(t, 0).start()

        @pl.when(sec > 0)
        def _():
            with jax.named_scope("wait_section"):
                section_copy(t, 1).wait_recv()

        steps([(1, there + 1, 0)])
        for m in (1, 0):
            steps([(0, there + m, n - 1)])
            with jax.named_scope("forward"):
                forward(there + m, m)
            if m == 1:
                steps([(1, there + 1, d) for d in far[:1]])

        @pl.when(sec < sections - 1)
        def _():
            with jax.named_scope("wait_section"):
                section_copy(t, 0).wait_recv()

        steps([(1, there + 1, d) for d in far[1:-1]])
        steps([(1, there, 0), (1, there + 1, n - 1)])
        with jax.named_scope("backward"):
            backward(there + 1, 1)
        for d in far[:-1]:
            steps([(1, there, d)])
            if t + 2 == ticks:
                sums(there + 1, d)
        steps([(1, there, n - 1)])
        with jax.named_scope("backward"):
            backward(there, 0)

    last = 2 * (ticks - 1)

    def grads_of(m):
        with jax.named_scope("wait_dp"):
            for t in range(ticks):
                for which in range(4):
                    for j in others:
                        dp_copy(which, 2 * t + m, j).wait_recv()
        with jax.named_scope("weight_grads"):
            weight_grads(m)

    sums(last, *far[:-2])
    finish(last + 1, 1)
    grads_of(1)
    sums(last, *far[-2:-1])
    finish(last, 0)
    for a in range(n):
        for b in range(reps):
            if a or b:
                gain_copy(a, b).start()
    grads_of(0)
    total = gtot[...]
    for a in range(n):
        for b in range(reps):
            if a or b:
                gain_copy(a, b).wait_recv()
                total = total + grecv[a * reps + b]
    gain_out[...] = total
    for u in range(units):
        sums_sent(u)
        for d in range(n - 1):
            for which in (0, 1):
                hand_on(which, u, d, lambda c: c.wait_send())
        for j in others:
            for which in range(4):
                dp_copy(which, u, j).wait_send()
    for t in range(ticks - 1):

        @pl.when(sec < sections - 1)
        def _():
            section_copy(t, 1).wait_send()

        @pl.when(sec > 0)
        def _():
            section_copy(t, 0).wait_send()

    for a in range(n):
        for b in range(reps):
            if a or b:
                gain_copy(a, b).wait_send()


def local(layer_in, carry_in, top_grad, w_qkv, w_out, gain):
    ticks, own, width = layer_in.shape[0], layer_in.shape[4], layer_in.shape[5]
    n = lax.axis_size("tensor")
    reps = lax.axis_size("dp")
    sections = lax.axis_size("section")
    cols, hq = w_qkv.shape[3], w_out.shape[2]
    if (width // reps) % 128 or (hq // reps) % 128 or ticks < 2:
        return local_permutes(layer_in, carry_in, top_grad, w_qkv, w_out, gain)
    length = n * own
    units = 2 * ticks
    groups = hq // (GROUP * HD)
    wn, wa = width // reps, hq // reps
    f32, bf16 = jnp.float32, jnp.bfloat16
    me = lax.axis_index("tensor")
    owners = (me + jnp.arange(n)) % n
    positions = (owners[:, None] * own + jnp.arange(own)[None, :]).reshape(-1)
    cosine, sine = rope_tables(positions, HD)
    slots = cols // HD
    cosine = jnp.tile(jnp.concatenate([cosine, cosine], axis=1), (1, slots))
    sine = jnp.tile(jnp.concatenate([-sine, sine], axis=1), (1, slots))
    bias = jnp.where(positions[:, None] >= positions[None, :], 0.0, -1e30).astype(f32)
    rows = layer_in[:, :, 0, 0]
    wide = rows.astype(f32)
    inverse = lax.rsqrt(jnp.mean(wide * wide, axis=-1, keepdims=True) + epsilon)
    normed = (wide * inverse * gain[:, 0][None, :, None, :]).astype(bf16)
    vmem = pl.BlockSpec(memory_space=pltpu.VMEM)
    hbm = pl.BlockSpec(memory_space=pl.ANY)
    dma = pltpu.SemaphoreType.DMA
    outs = pl.pallas_call(
        functools.partial(fused, n, reps, ticks, sections, own),
        out_shape=(
            jax.ShapeDtypeStruct((units, own, width), bf16),
            jax.ShapeDtypeStruct((2, wn, cols), bf16),
            jax.ShapeDtypeStruct((2, wa, width), bf16),
            jax.ShapeDtypeStruct((2, 1, width), f32),
        ),
        in_specs=[vmem] * 5 + [hbm] * 2 + [vmem] * 3,
        out_specs=(vmem,) * 4,
        scratch_shapes=[
            pltpu.VMEM((2, width, cols), bf16),
            pltpu.VMEM((2, hq, width), bf16),
            pltpu.VMEM((units, length, width), bf16),
            pltpu.VMEM((units, length, width), bf16),
            pltpu.VMEM((units, length, cols), bf16),
            pltpu.VMEM((units, length, hq), bf16),
            pltpu.VMEM((units, reps - 1, length, wn), bf16),
            pltpu.VMEM((units, reps - 1, length, width), bf16),
            pltpu.VMEM((units, reps - 1, length, cols), bf16),
            pltpu.VMEM((units, reps - 1, length, wa), bf16),
            pltpu.VMEM((units, length, width), bf16),
            pltpu.VMEM((units, 2, n - 1, own, width), bf16),
            pltpu.VMEM((units, groups, GROUP * length, length), f32),
            pltpu.VMEM((units, groups, GROUP * length, HD), bf16),
            pltpu.VMEM((units, groups, length, HD), bf16),
            pltpu.VMEM((units, groups, length, HD), bf16),
            pltpu.VMEM((2, 1, width), f32),
            pltpu.VMEM((n * reps, 2, 1, width), f32),
            pltpu.VMEM((own, width), f32),
            dma((2, 2)),
            dma((units + 2,)),
            dma((2, units, 2 * n)),
            dma((2, units, n)),
            dma((units, 2, n)),
            dma((units, 2, n)),
            dma((ticks, 2)),
            dma((ticks, 2)),
            dma((4, units, reps)),
            dma((4, units, reps)),
            dma((n * reps,)),
            dma((n * reps,)),
        ],
        compiler_params=pltpu.CompilerParams(
            collective_id=0, has_side_effects=True, vmem_limit_bytes=64 * 1024 * 1024 - 65536
        ),
    )(
        normed.reshape(units, own, width),
        rows.reshape(units, own, width),
        carry_in[:, 0, 0],
        top_grad[:, 0],
        gain,
        w_qkv[:, 0],
        w_out[:, 0],
        cosine,
        sine,
        bias,
    )
    return (
        outs[0].reshape(ticks, 2, 1, 1, own, width),
        outs[1][:, None],
        outs[2][:, None],
        outs[3],
    )


def solution(mesh):
    in_specs = (
        P(None, None, "section", "dp", "tensor", None),
        P(None, "section", "dp", "tensor", None),
        P(None, "dp", "tensor", None),
        P(None, "section", None, "tensor"),
        P(None, "section", "tensor", None),
        P(None, "section", None),
    )
    out_specs = (
        P(None, None, "section", "dp", "tensor", None),
        P(None, "section", "dp", "tensor"),
        P(None, "section", ("tensor", "dp"), None),
        P(None, "section", None),
    )
    return jax.shard_map(local, mesh=mesh, in_specs=in_specs, out_specs=out_specs, check_vma=False)
```
